32 devices in a mesh: dp: 2 (over x), sw: 4 (over z), sh: 4 (over y, core).
Axes of the slice: x: 2, y: 2, z: 4, core: 2. Of those that a mesh axis runs over, the one named last changes fastest.
Arguments:
- features: bfloat16 [2, 256, 12, 24, 96], P('dp', None, None, 'sh', 'sw'), parts along dimension 0
- latent: bfloat16 [2, 16, 12, 24, 96], P('dp', None, None, 'sh', 'sw'), parts along dimension 0
- gn_gain: float32 [2, 2, 256], replicated
- gn_bias: float32 [2, 2, 256], replicated
- zy_weight: bfloat16 [2, 2, 16, 256], replicated
- zy_bias: float32 [2, 2, 256], replicated
- zb_weight: bfloat16 [2, 2, 16, 256], replicated
- zb_bias: float32 [2, 2, 256], replicated
- conv_weight: bfloat16 [2, 2, 256, 256, 3, 3, 3], replicated
- conv_bias: float32 [2, 2, 256], replicated
- up_weight: bfloat16 [256, 256, 3, 3], replicated
- up_bias: float32 [256], replicated
Outputs:
- output: bfloat16 [2, 256, 12, 48, 192], P('dp', None, None, 'sh', 'sw'), parts along dimension 0
There are 2 independent parts. The reference program is written for one: setup_inputs(seed, part) draws one part's arguments, and reference() takes and returns one part's arrays. A program takes and returns all parts, laid end to end along the dimension named above; an argument that names none is the same for every part.
All inputs are finite; a program needn't handle non-finite values.
Results may differ from the reference program's by a relative error of at most 0.013683.
Values are sent between devices in bfloat16 or wider.
A program may use at most 1 GiB of HBM per device.

```python
import jax
import jax.numpy as jnp
from jax import lax

CHANNELS = 256
LATENT = 16
GROUPS = 32
RES_BLOCKS = 2
FRAMES = 12
HEIGHT = 24
WIDTH = 96
GN_EPSILON = 1e-6
CONV_DIMS = ("NCDHW", "OIDHW", "NCDHW")


def setup_inputs(seed: int = 0, part: int = 0) -> dict:
    part_key = jax.random.fold_in(jax.random.key(seed), part)
    data_keys = jax.random.split(part_key, 6)
    weight_keys = jax.random.split(jax.random.key(seed + 1), 10)
    ramp_h = jnp.linspace(-1.0, 1.0, HEIGHT)[:, None]
    ramp_w = jnp.linspace(-1.0, 1.0, WIDTH)[None, :]
    amp_rows = jax.random.normal(data_keys[0], (CHANNELS, 1, 1, 1), jnp.float32)
    amp_cols = jax.random.normal(data_keys[1], (CHANNELS, 1, 1, 1), jnp.float32)
    noise = jax.random.normal(data_keys[2], (CHANNELS, FRAMES, HEIGHT, WIDTH), jnp.float32)
    features = (noise + amp_rows * ramp_h + amp_cols * ramp_w)[None].astype(jnp.bfloat16)
    lat_rows = jax.random.normal(data_keys[3], (LATENT, 1, 1, 1), jnp.float32)
    lat_cols = jax.random.normal(data_keys[4], (LATENT, 1, 1, 1), jnp.float32)
    lat_noise = jax.random.normal(data_keys[5], (LATENT, FRAMES, HEIGHT, WIDTH), jnp.float32)
    latent = (lat_noise + lat_rows * ramp_h + lat_cols * ramp_w)[None].astype(jnp.bfloat16)
    vec_shape = (RES_BLOCKS, 2, CHANNELS)
    map_shape = (RES_BLOCKS, 2, LATENT, CHANNELS)
    gn_gain = 1.0 + 0.3 * jax.random.normal(weight_keys[0], vec_shape, jnp.float32)
    gn_bias = 0.3 * jax.random.normal(weight_keys[1], vec_shape, jnp.float32)
    zy_weight = (jax.random.normal(weight_keys[2], map_shape, jnp.float32) * (0.5 * LATENT ** -0.5)).astype(jnp.bfloat16)
    zy_bias = 1.0 + 0.3 * jax.random.normal(weight_keys[3], vec_shape, jnp.float32)
    zb_weight = (jax.random.normal(weight_keys[4], map_shape, jnp.float32) * (0.5 * LATENT ** -0.5)).astype(jnp.bfloat16)
    zb_bias = 0.3 * jax.random.normal(weight_keys[5], vec_shape, jnp.float32)
    conv_weight = (jax.random.normal(weight_keys[6], (RES_BLOCKS, 2, CHANNELS, CHANNELS, 3, 3, 3), jnp.float32) * (27 * CHANNELS) ** -0.5).astype(jnp.bfloat16)
    conv_bias = 0.3 * jax.random.normal(weight_keys[7], vec_shape, jnp.float32)
    up_weight = (jax.random.normal(weight_keys[8], (CHANNELS, CHANNELS, 3, 3), jnp.float32) * (9 * CHANNELS) ** -0.5).astype(jnp.bfloat16)
    up_bias = 0.3 * jax.random.normal(weight_keys[9], (CHANNELS,), jnp.float32)
    return {"features": features, "latent": latent, "gn_gain": gn_gain, "gn_bias": gn_bias, "zy_weight": zy_weight, "zy_bias": zy_bias, "zb_weight": zb_weight, "zb_bias": zb_bias, "conv_weight": conv_weight, "conv_bias": conv_bias, "up_weight": up_weight, "up_bias": up_bias}


def per_channel(values):
    return values[None, :, None, None, None]


def group_norm(values, gain, shift):
    grouped = values.astype(jnp.float32).reshape(1, GROUPS, CHANNELS // GROUPS, FRAMES, HEIGHT, WIDTH)
    group_mean = jnp.mean(grouped, axis=(2, 3, 4, 5), keepdims=True)
    group_var = jnp.mean(jnp.square(grouped - group_mean), axis=(2, 3, 4, 5), keepdims=True)
    normed = ((grouped - group_mean) * lax.rsqrt(group_var + GN_EPSILON)).reshape(1, CHANNELS, FRAMES, HEIGHT, WIDTH)
    return normed * per_channel(gain) + per_channel(shift)


def latent_map(latent, weight, bias):
    return jnp.einsum("nzthw,zc->ncthw", latent.astype(jnp.float32), weight.astype(jnp.float32)) + per_channel(bias)


def causal_conv(activated, weight, bias):
    first_frame = activated[:, :, :1]
    padded = jnp.concatenate([first_frame, first_frame, activated], axis=2)
    padded = jnp.pad(padded, ((0, 0), (0, 0), (0, 0), (1, 1), (1, 1)))
    conv_out = lax.conv_general_dilated(padded.astype(jnp.float32), weight.astype(jnp.float32), (1, 1, 1), "VALID", dimension_numbers=CONV_DIMS)
    return (conv_out + per_channel(bias)).astype(jnp.bfloat16)


def reference(features, latent, gn_gain, gn_bias, zy_weight, zy_bias, zb_weight, zb_bias, conv_weight, conv_bias, up_weight, up_bias):
    hidden = features
    for block in range(RES_BLOCKS):
        branch = hidden
        for slot in range(2):
            normed = group_norm(branch, gn_gain[block, slot], gn_bias[block, slot])
            mixed = normed * latent_map(latent, zy_weight[block, slot], zy_bias[block, slot]) + latent_map(latent, zb_weight[block, slot], zb_bias[block, slot])
            activated = jax.nn.silu(mixed).astype(jnp.bfloat16)
            branch = causal_conv(activated, conv_weight[block, slot], conv_bias[block, slot])
        hidden = (hidden.astype(jnp.float32) + branch.astype(jnp.float32)).astype(jnp.bfloat16)
    upsampled = jnp.repeat(jnp.repeat(hidden, 2, axis=3), 2, axis=4)
    padded = jnp.pad(upsampled, ((0, 0), (0, 0), (0, 0), (1, 1), (1, 1)))
    conv_out = lax.conv_general_dilated(padded.astype(jnp.float32), up_weight[:, :, None].astype(jnp.float32), (1, 1, 1), "VALID", dimension_numbers=CONV_DIMS)
    return (conv_out + per_channel(up_bias)).astype(jnp.bfloat16)
```

```python
import functools

import jax
import jax.numpy as jnp
from jax import lax
from jax.experimental import pallas as pl
from jax.experimental.pallas import tpu as pltpu
from jax.sharding import PartitionSpec as P

GN_EPSILON = 1e-6
MESH = pl.DeviceIdType.MESH
F32 = jnp.float32
CONTRACT_LAST = (((1,), (1,)), ((), ()))
BF16 = jnp.bfloat16
T, H, W, C, LZ = 12, 6, 24, 256, 16
HE = H + 2
FR = T * W
NA, NB = T * 16, T * 8
AR = (T + 2) * 16 + (T // 2 + 2) * 16
ABASE = (T + 2) * 16
SW_ = 40
T2 = T // 2


LN = 128
PAIR = range(2)
TR = 16


def lanes(half):
    return pl.ds(half * LN, LN)


def tile(i):
    return pl.ds(i * TR, TR)


def chan(ref, b, s):
    return ref[b, pl.ds(s, 1), :]


def acc_specs():
    specs = []
    for q in PAIR:
        for _ in range(3):
            specs += [pltpu.ACC(q)((NA, C), F32), pltpu.ACC(q)((NB, C), F32)]
    return specs


def write_operand(a_ref, s_ref, h):
    for half in PAIR:
        ln = lanes(half)
        for kw in range(3):
            tails = []
            for t in range(T):
                body = s_ref[half, pl.ds(t * SW_ + 7 + kw, 16), :].astype(BF16)
                a_ref[kw, h, tile(t + 2), ln] = body
                if t == 0:
                    a_ref[kw, h, tile(0), ln] = body
                    a_ref[kw, h, tile(1), ln] = body
                tails.append(s_ref[half, pl.ds(t * SW_ + 23 + kw, 8), :])
            pairs = [(max(t, 0), t + T2) for t in range(-2, T2)]
            for i, (p, n) in enumerate(pairs):
                both = jnp.concatenate([tails[p], tails[n]], axis=0).astype(BF16)
                a_ref[kw, h, pl.ds(ABASE + i * TR, TR), ln] = both


def stage_kernel(n_sh, n_sw, feat, lat, gain, gbias, zyw, zyb, zbw, zbb, cw, cb,
                 xe_out, ce_out,
                 wv, a_ref, rx, xres, cv, yv, bv, lt, ltf, lv, fb, re, ce, rs, cs, lts, sv, wz,
                 stat_out, stat_in, par,
                 ld_sem, w_sem, hs_sem, hr_sem, ls_sem, lr_sem, ss_sem, sr_sem):
    n_dev = n_sh * n_sw
    sh = lax.axis_index("sh")
    sw = lax.axis_index("sw")
    me = sh * n_sw + sw
    has = {"u": sh > 0, "d": sh < n_sh - 1, "l": sw > 0, "r": sw < n_sw - 1}

    ld_feat = pltpu.make_async_copy(feat, fb, ld_sem.at[0])
    ld_lat = pltpu.make_async_copy(lat, lv, ld_sem.at[1])
    ld_feat.start()
    ld_lat.start()

    def ld_weight(n, b, s):
        return pltpu.make_async_copy(cw.at[b, s], wv.at[n], w_sem.at[n])

    for n in range(4):
        ld_weight(n, n // 2, n % 2).start()

    zero_rows = jnp.zeros((FR, 128), BF16)
    for i in (0, HE - 1, HE):
        lt[i] = zero_rows

    def peer_of(j):
        p = lax.rem(me + j, n_dev)
        return p, {"sh": p // n_sw, "sw": lax.rem(p, n_sw)}

    bar = pltpu.get_barrier_semaphore()
    for j in range(1, n_dev):
        pl.semaphore_signal(bar, inc=1, device_id=peer_of(j)[1], device_id_type=MESH)

    dirs = [(-1, 0), (1, 0), (0, -1), (0, 1), (-1, -1), (-1, 1), (1, -1), (1, 1)]

    def exists(dy, dx):
        c = None
        for cond, use in ((has["u"], dy < 0), (has["d"], dy > 0), (has["l"], dx < 0), (has["r"], dx > 0)):
            if use:
                c = cond if c is None else jnp.logical_and(c, cond)
        return c

    def device(dy, dx):
        return {"sh": sh + dy, "sw": sw + dx}

    def halo_refs(e, dy, dx, src0):
        side = 1 if dx < 0 else 0
        row = HE - 1 if dy < 0 else 0
        if dx == 0:
            src = (src0[0] if dy < 0 else src0[1])
            return src, re.at[e, 1 if dy < 0 else 0]
        col = 0 if dx < 0 else 1
        if dy == 0:
            return cs.at[col], ce.at[e, side, pl.ds(1, H)]
        return cs.at[col, 0 if dy < 0 else H - 1], ce.at[e, side, row]

    def halo_copy(e, d, src0):
        dy, dx = dirs[d]
        src, dst = halo_refs(e, dy, dx, src0)
        return pltpu.make_async_remote_copy(src_ref=src, dst_ref=dst, send_sem=hs_sem.at[e, d],
                                            recv_sem=hr_sem.at[e, d], device_id=device(dy, dx), device_id_type=MESH)

    def lat_copy(d):
        dy, dx = dirs[d]
        if dx == 0:
            src, dst = (lt.at[1], lt.at[HE - 1]) if dy < 0 else (lt.at[H], lt.at[0])
        else:
            col = 0 if dx < 0 else 1
            base = 128 if dx < 0 else 0
            if dy == 0:
                src, dst = lts.at[col], lt.at[HE, pl.ds(base + 16, H * 16)]
            else:
                row = 0 if dy < 0 else H - 1
                there = (HE - 1 if dy < 0 else 0) * 16
                src, dst = lts.at[col, tile(row)], lt.at[HE, pl.ds(base + there, 16)]
        return pltpu.make_async_remote_copy(src_ref=src, dst_ref=dst, send_sem=ls_sem.at[d],
                                            recv_sem=lr_sem.at[d], device_id=device(dy, dx), device_id_type=MESH)

    def for_dirs(make, what):
        for d, (dy, dx) in enumerate(dirs):
            if what == "recv":
                @pl.when(exists(-dy, -dx))
                def _(d=d):
                    make(d).wait_recv()
            else:
                @pl.when(exists(dy, dx))
                def _(d=d):
                    if what == "start":
                        make(d).start()
                    else:
                        make(d).wait_send()

    def stat_copy(n, j):
        p, dev = peer_of(j)
        return pltpu.make_async_remote_copy(src_ref=stat_out.at[n], dst_ref=stat_in.at[n, me], send_sem=ss_sem.at[n, j],
                                            recv_sem=sr_sem.at[n, me], device_id=dev, device_id_type=MESH)

    def send_stats(n, pivot, s1, s2):
        count = float(T * H * W)
        s1 = jnp.sum(s1, axis=0, keepdims=True) * (1.0 / count)
        s2 = jnp.sum(s2, axis=0, keepdims=True) * (1.0 / count)
        mean = pivot + s1
        var = jnp.maximum(s2 - s1 * s1, 0.0)
        rows = [mean[:, :128], mean[:, 128:], var[:, :128], var[:, 128:]]
        packed = jnp.concatenate(rows + [jnp.zeros((4, 128), F32)], axis=0)
        stat_out[n] = packed
        stat_in[n, me] = packed
        for j in range(1, n_dev):
            stat_copy(n, j).start()

    def recv_stats(n, b, s):
        for j in range(1, n_dev):
            p = lax.rem(me + j, n_dev)
            pltpu.make_async_remote_copy(src_ref=stat_out.at[n], dst_ref=stat_in.at[n, p], send_sem=ss_sem.at[n, j],
                                         recv_sem=sr_sem.at[n, p], device_id=peer_of(j)[1], device_id_type=MESH).wait_recv()
        vals = [stat_in[n, i] for i in range(n_dev)]
        total = functools.reduce(jnp.add, vals) * (1.0 / n_dev)
        mean = total[0:2, :]
        dev = functools.reduce(jnp.add, [jnp.square(v[0:2, :] - mean) for v in vals]) * (1.0 / n_dev)
        var = total[2:4, :] + dev
        lane = lax.broadcasted_iota(jnp.int32, (2, 128), 1)
        for gap in (1, 2, 4):
            low = (lane & gap) == 0

            def partner(v):
                return jnp.where(low, pltpu.roll(v, LN - gap, 1), pltpu.roll(v, gap, 1))

            mp, vp = partner(mean), partner(var)
            half_gap = (mean - mp) * 0.5
            var = (var + vp) * 0.5 + half_gap * half_gap
            mean = (mean + mp) * 0.5
        rstd = lax.rsqrt(var + GN_EPSILON)
        mean = jnp.concatenate([mean[0:1], mean[1:2]], axis=1)
        rstd = jnp.concatenate([rstd[0:1], rstd[1:2]], axis=1)
        par[0] = jnp.broadcast_to(mean, (8, C))
        par[1] = jnp.broadcast_to(rstd * chan(gain, b, s), (8, C))
        par[2] = jnp.broadcast_to(chan(gbias, b, s), (8, C))

    def fill_columns():
        for h in range(H):
            for side, w in ((0, 0), (1, W - 1)):
                for half in PAIR:
                    v = rx[half, pl.ds((h + 1) * FR + w, 16, stride=W), :]
                    cs[side, h, :, lanes(half)] = v.astype(BF16)

    def main():
        ld_feat.wait()
        pivot0 = fb[0, 0, pl.ds(0, 8), :].astype(F32)[0:1, :]
        pivot8 = jnp.broadcast_to(pivot0, (8, C))

        def load_row(h, carry):
            s1, s2 = carry
            for t in range(T):
                x = fb[t, h].astype(F32)
                for half in PAIR:
                    rx[half, pl.ds((h + 1) * FR + t * W, W), :] = x[:, half * LN:half * LN + LN]
                xres[h, pl.ds(t * W, W), :] = x
                for i in range(3):
                    d = x[i * 8:i * 8 + 8] - pivot8
                    s1 = s1 + d
                    s2 = s2 + d * d
            return s1, s2

        zero8 = jnp.zeros((8, C), F32)
        s1, s2 = lax.fori_loop(0, H, load_row, (zero8, zero8))
        for t in range(T):
            rs[0, t] = fb[t, 0]
            rs[1, t] = fb[t, H - 1]
        fill_columns()
        pl.semaphore_wait(bar, n_dev - 1)
        send_stats(0, pivot0, s1, s2)
        row_src = (rs.at[0], rs.at[1])
        for_dirs(lambda d: halo_copy(0, d, row_src), "start")

        ltf[...] = jnp.zeros(ltf.shape, F32)
        ld_lat.wait()

        def turn_row(h, c):
            for t in range(T):
                ltf[pl.ds(h * FR + t * W, W), pl.ds(0, LZ)] = lv[t, h].astype(F32).T
            row = ltf[pl.ds(pl.multiple_of(h * FR, 16), FR), :].astype(BF16)
            lt[h + 1] = row
            return c

        lax.fori_loop(0, H, turn_row, 0)
        for h in range(H):
            for side, w in ((0, 0), (1, W - 1)):
                lts[side, tile(h), :] = ltf[pl.ds(h * FR + w, 16, stride=W), :].astype(BF16)
        for_dirs(lat_copy, "start")
        wz[...] = jnp.zeros(wz.shape, BF16)
        for_dirs(lat_copy, "recv")
        for_dirs(lat_copy, "send")

        half_or_zero = {k: jnp.where(v, 0.5, 0.0).astype(F32) for k, v in has.items()}

        def latent_maps(b, s):
            wz[pl.ds(0, LZ), pl.ds(0, C)] = zyw[b, s]
            wz[pl.ds(0, LZ), pl.ds(C, C)] = zbw[b, s]
            biases = (chan(zyb, b, s), chan(zbb, b, s))
            for i in range(HE + 1):
                v = jnp.dot(lt[i], wz[...], preferred_element_type=F32)
                for q, out in ((0, yv), (1, bv)):
                    m = v[:, q * C:q * C + C] + biases[q]
                    if i < HE:
                        f = half_or_zero["u"] if i == 0 else half_or_zero["d"] if i == HE - 1 else 0.5
                        out[i] = m * f
                    else:
                        for seg in range(2 * HE):
                            f = half_or_zero["l" if seg < HE else "r"]
                            if seg % HE == 0:
                                f = f * half_or_zero["u"] * 2.0
                            if seg % HE == HE - 1:
                                f = f * half_or_zero["d"] * 2.0
                            out[i, tile(seg), :] = m[seg * TR:seg * TR + TR] * f

        def activate(x, y, b):
            n = x.shape[0] // 8
            x, y, b = (v.reshape(n, 8, C) for v in (x, y, b))
            hv = ((x - par[0][None]) * par[1][None] + par[2][None]) * y + b
            return (hv * jnp.tanh(hv) + hv).reshape(n * 8, C)

        def halo_rows(e):
            for i, cond in ((0, has["u"]), (1, has["d"])):
                row = 0 if i == 0 else HE - 1
                for t in range(T):
                    v = jnp.where(cond, re[e, i, t].astype(F32), 0.0)
                    for half in PAIR:
                        rx[half, pl.ds(row * FR + t * W, W), :] = v[:, half * LN:half * LN + LN]

        def col_vals(e, side, h):
            cond = has["l"] if side == 0 else has["r"]
            cond = jnp.logical_and(cond, jnp.logical_or(h > 0, has["u"]))
            cond = jnp.logical_and(cond, jnp.logical_or(h < HE - 1, has["d"]))
            return jnp.where(cond, ce[e, side, h].astype(F32), 0.0)

        def activate_rows(n):
            def row(h, c):
                for side in PAIR:
                    k = side * 128 + h * 16
                    v = activate(col_vals(n, side, h), yv[HE, pl.ds(pl.multiple_of(k, TR), TR), :], bv[HE, pl.ds(pl.multiple_of(k, TR), TR), :])
                    for half in PAIR:
                        sv[half, pl.ds(7 + side * 25, T, stride=SW_), :] = v[0:T, half * LN:half * LN + LN]
                for t in range(T):
                    x = jnp.concatenate([rx[half, pl.ds(pl.multiple_of(h * FR, 8) + t * W, W), :] for half in PAIR], axis=1)
                    v = activate(x, yv[h, pl.ds(t * W, W), :], bv[h, pl.ds(t * W, W), :])
                    for half in PAIR:
                        sv[half, pl.ds(t * SW_ + 8, W), :] = v[:, half * LN:half * LN + LN]
                write_operand(a_ref, sv, h)
                return c

            lax.fori_loop(0, HE, row, 0)

        def conv(n):
            def lhs(h, part, tap):
                kt, kh, kw = tap // 9, tap // 3 % 3, tap % 3
                return a_ref[kw, h + kh, pl.ds(kt * 16 + (ABASE if part else 0), NB if part else NA), :]

            for i in range(9):
                rhs = jnp.concatenate([wv[n, i * 3 + kw] for kw in range(3)], axis=1)
                for h in range(H):
                    cols = [jnp.concatenate([lhs(h, part, i * 3 + kw) for part in PAIR], axis=0) for kw in range(3)]
                    v = lax.dot_general(jnp.concatenate(cols, axis=1), rhs, CONTRACT_LAST, preferred_element_type=F32)
                    if i == 0:
                        cv[h] = v
                    else:
                        cv[h] += v

        def finish(b, s):
            bias = chan(cb, b, s)
            pivot = None
            s1 = s2 = zero8
            for hh in range(3):
                for q in PAIR:
                    h = q * 3 + hh
                    for part in PAIR:
                        v = (cv[h, pl.ds(NA if part else 0, NB if part else NA), :] + bias).astype(BF16).astype(F32)
                        nblk = 16 if part == 0 else 8
                        for i in range(T):
                            if part == 0:
                                t, w0 = i, 0
                            else:
                                t, w0 = (i // 2) + (i % 2) * T2, 16
                            blk = v[i * nblk:(i + 1) * nblk]
                            r0 = t * W + w0
                            if s == 1:
                                blk = (blk + xres[h, pl.ds(r0, nblk), :]).astype(BF16).astype(F32)
                                xres[h, pl.ds(r0, nblk), :] = blk
                            for half in PAIR:
                                rx[half, pl.ds((h + 1) * FR + r0, nblk), :] = blk[:, half * LN:half * LN + LN]
                            if h in (0, H - 1):
                                rs[0 if h == 0 else 1, t, pl.ds(w0, nblk), :] = blk.astype(BF16)
                            if s == 1:
                                xe_out[h + 1, t, pl.ds(w0, nblk), :] = blk.astype(BF16)
                            if pivot is None:
                                pivot = blk[0:1, :]
                            for k in range(nblk // 8):
                                d = blk[k * 8:k * 8 + 8] - pivot
                                s1 = s1 + d
                                s2 = s2 + d * d
            return pivot, s1, s2

        def block(b, carry):
            for s in PAIR:
                n = b * 2 + s
                latent_maps(b, s)
                for_dirs(lambda d: halo_copy(n, d, row_src), "recv")
                halo_rows(n)
                recv_stats(n, b, s)
                activate_rows(n)
                ld_weight(n, b, s).wait()
                conv(n)
                for_dirs(lambda d: halo_copy(n, d, row_src), "send")
                pivot, s1, s2 = finish(b, s)
                if s == 0:
                    send_stats(n + 1, pivot, s1, s2)
                else:
                    @pl.when(b == 0)
                    def _():
                        send_stats(n + 1, pivot, s1, s2)
                fill_columns()
                for_dirs(lambda d: halo_copy(n + 1, d, row_src), "start")
            return carry

        lax.fori_loop(0, 2, block, 0)

        for_dirs(lambda d: halo_copy(4, d, row_src), "recv")
        for i, cond in ((0, has["u"]), (1, has["d"])):
            row = 0 if i == 0 else HE - 1
            for t in range(T):
                xe_out[row, t] = jnp.where(cond, re[4, i, t].astype(F32), 0.0).astype(BF16)
        for side in PAIR:
            for h in range(HE):
                ce_out[side, h] = col_vals(4, side, h).astype(BF16)
        for_dirs(lambda d: halo_copy(4, d, row_src), "send")
        for n in range(4):
            for j in range(1, n_dev):
                stat_copy(n, j).wait_send()

    main()


def up_kernel(xe, ce, wu, ub, out, a_ref, sv, o32, ob, o_sem):
    def row(h, c):
        for side in PAIR:
            v = ce[side, h].astype(F32)
            for half in PAIR:
                sv[half, pl.ds(7 + side * 25, T, stride=SW_), :] = v[0:T, half * LN:half * LN + LN]
        for t in range(T):
            v = xe[h, t].astype(F32)
            for half in PAIR:
                sv[half, pl.ds(t * SW_ + 8, W), :] = v[:, half * LN:half * LN + LN]
        write_operand(a_ref, sv, h)
        return c

    lax.fori_loop(0, HE, row, 0)

    def out_copy(q, a, hp):
        return pltpu.make_async_copy(ob.at[q, a], out.at[:, 2 * (q * 3 + hp) + a], o_sem.at[q, a])

    def main(*accs):
        for acc in accs:
            pltpu.matmul_pop(acc)
        taps = [(a, b, k, l) for a in PAIR for b in PAIR for k in range(3) for l in range(3)]

        def push(i):
            _, _, k, l = taps[i]
            for q in PAIR:
                pltpu.matmul_push_rhs(wu[k, l], staging_register=0, mxu_index=q, transpose=True)

        def third(hp, c):
            push(0)
            for i, (a, b, k, l) in enumerate(taps):
                ph = (a * 2 + b) % 3
                dh = (a + k + 1) // 2
                kw = (b + l + 1) // 2
                for q in PAIR:
                    h = q * 3 + hp + dh
                    pltpu.matmul_acc_lhs(accs[q * 6 + ph * 2], a_ref[kw, h, pl.ds(32, NA), :], load_staged_rhs=0)
                    if i + 1 < len(taps):
                        _, _, k2, l2 = taps[i + 1]
                        pltpu.matmul_push_rhs(wu[k2, l2], staging_register=0, mxu_index=q, transpose=True)
                    pltpu.matmul_acc_lhs(accs[q * 6 + ph * 2 + 1], a_ref[kw, h, pl.ds(ABASE + 32, NB), :])
                if (k, l) != (2, 2):
                    continue
                for q in PAIR:
                    va = pltpu.matmul_pop(accs[q * 6 + ph * 2]) + ub[...]
                    vb = pltpu.matmul_pop(accs[q * 6 + ph * 2 + 1]) + ub[...]
                    for half in PAIR:
                        ln = slice(half * 128, half * 128 + 128)
                        for t in range(T):
                            o32[q, half, pl.ds(t * 48 + b, 16, stride=2), :] = va[t * 16:t * 16 + 16, ln]
                            kb = (t % T2) * 16 + (t // T2) * 8
                            o32[q, half, pl.ds(t * 48 + 32 + b, 8, stride=2), :] = vb[kb:kb + 8, ln]
                    if b == 1:
                        @pl.when(hp > 0)
                        def _(q=q, a=a):
                            out_copy(q, a, hp - 1).wait()
                        for t in range(T):
                            for half in PAIR:
                                ob[q, a, t, :, lanes(half)] = o32[q, half, pl.ds(t * 48, 48), :].astype(BF16)
                        out_copy(q, a, hp).start()
            return c

        lax.fori_loop(0, 3, third, 0)
        for q in PAIR:
            for a in PAIR:
                out_copy(q, a, 2).wait()

    pl.run_scoped(main, *acc_specs())


def solution(mesh):
    n_sh, n_sw = mesh.shape["sh"], mesh.shape["sw"]
    n_dev = n_sh * n_sw
    vmem = pl.BlockSpec(memory_space=pltpu.VMEM)
    hbm = pl.BlockSpec(memory_space=pl.ANY)
    dma = pltpu.SemaphoreType.DMA

    def local_step(features, latent, gn_gain, gn_bias, zy_weight, zy_bias, zb_weight, zb_bias, conv_weight, conv_bias, up_weight, up_bias):
        feat = features[0].transpose(1, 2, 3, 0)
        lat = latent[0].transpose(1, 2, 0, 3)
        cw = conv_weight.transpose(0, 1, 4, 5, 6, 2, 3).reshape(2, 2, 27, C, C)
        uw = up_weight.transpose(2, 3, 0, 1)
        xe, ce = pl.pallas_call(
            functools.partial(stage_kernel, n_sh, n_sw),
            out_shape=(jax.ShapeDtypeStruct((HE, T, W, C), BF16), jax.ShapeDtypeStruct((2, HE, 16, C), BF16)),
            in_specs=[hbm, hbm] + [vmem] * 6 + [hbm, vmem],
            out_specs=(vmem, vmem),
            scratch_shapes=[
                pltpu.VMEM((4, 27, C, C), BF16),
                pltpu.VMEM((3, HE, AR, C), BF16),
                pltpu.VMEM((2, HE * FR, 128), F32),
                pltpu.VMEM((H, FR, C), F32),
                pltpu.VMEM((H, FR, C), F32),
                pltpu.VMEM((HE + 1, FR, C), F32),
                pltpu.VMEM((HE + 1, FR, C), F32),
                pltpu.VMEM((HE + 1, FR, 128), BF16),
                pltpu.VMEM((H * FR + 96, 128), F32),
                pltpu.VMEM((T, H, LZ, W), BF16),
                pltpu.VMEM((T, H, W, C), BF16),
                pltpu.VMEM((5, 2, T, W, C), BF16),
                pltpu.VMEM((5, 2, HE, 16, C), BF16),
                pltpu.VMEM((2, T, W, C), BF16),
                pltpu.VMEM((2, H, 16, C), BF16),
                pltpu.VMEM((2, H * 16, 128), BF16),
                pltpu.VMEM((2, T * SW_, 128), F32),
                pltpu.VMEM((128, 2 * C), BF16),
                pltpu.VMEM((4, 8, 128), F32),
                pltpu.VMEM((4, n_dev, 8, 128), F32),
                pltpu.VMEM((3, 8, C), F32),
                dma((2,)), dma((4,)), dma((5, 8)), dma((5, 8)), dma((8,)), dma((8,)), dma((4, n_dev)), dma((4, n_dev)),
            ],
            compiler_params=pltpu.CompilerParams(collective_id=0, has_side_effects=True, vmem_limit_bytes=56 << 20),
            name="stages",
        )(feat, lat, gn_gain, gn_bias, zy_weight, zy_bias, zb_weight, zb_bias, cw, conv_bias)
        out = pl.pallas_call(
            up_kernel,
            out_shape=jax.ShapeDtypeStruct((T, 2 * H, 2 * W, C), BF16),
            in_specs=[vmem] * 4,
            out_specs=hbm,
            scratch_shapes=[
                pltpu.VMEM((3, HE, AR, C), BF16),
                pltpu.VMEM((2, T * SW_, 128), F32),
                pltpu.VMEM((2, 2, T * 2 * W, 128), F32),
                pltpu.VMEM((2, 2, T, 2 * W, C), BF16),
                dma((2, 2)),
            ],
            compiler_params=pltpu.CompilerParams(vmem_limit_bytes=40 << 20),
            name="upsample",
        )(xe, ce, uw, up_bias.reshape(1, C))
        return out.transpose(3, 0, 1, 2)[None]

    data_spec = P("dp", None, None, "sh", "sw")
    return jax.shard_map(local_step, mesh=mesh, in_specs=(data_spec, data_spec) + (P(),) * 10, out_specs=data_spec, check_vma=False)
```

```python
import functools

import jax
import jax.numpy as jnp
from jax import lax
from jax.experimental import pallas as pl
from jax.experimental.pallas import tpu as pltpu
from jax.sharding import PartitionSpec as P

GN_EPSILON = 1e-6
MESH = pl.DeviceIdType.MESH
F32 = jnp.float32
CONTRACT_LAST = (((1,), (1,)), ((), ()))
BF16 = jnp.bfloat16
T, H, W, C, LZ = 12, 6, 24, 256, 16
HE = H + 2
FR = T * W
NA, NB = T * 16, T * 8
AR = (T + 2) * 16 + (T // 2 + 2) * 16
ABASE = (T + 2) * 16
SW_ = 40
T2 = T // 2
dirs = [(-1, 0), (1, 0), (0, -1), (0, 1), (-1, -1), (-1, 1), (1, -1), (1, 1)]
ROW_DIRS, COL_DIRS = (0, 1, 4, 5, 6, 7), (2, 3)
EDGE, INNER = (0, H - 1), range(1, H - 1)


LN = 128
PAIR, TRIO = range(2), range(3)
TR, SUB = 16, 8


def lanes(half):
    return pl.ds(half * LN, LN)


def tile(i):
    return pl.ds(i * TR, TR)


def chan(ref, b, s):
    return ref[b, pl.ds(s, 1), :]


def acc_specs():
    specs = []
    for q in PAIR:
        for _ in TRIO:
            specs += [pltpu.ACC(q)((NA, C), F32), pltpu.ACC(q)((NB, C), F32)]
    return specs


def write_operand(a_ref, s_ref, h):
    for half in PAIR:
        ln = lanes(half)
        for kw in TRIO:
            tails = []
            for t in range(T):
                body = s_ref[half, pl.ds(t * SW_ + 7 + kw, 16), :].astype(BF16)
                a_ref[kw, h, tile(t + 2), ln] = body
                if t == 0:
                    a_ref[kw, h, tile(0), ln] = body
                    a_ref[kw, h, tile(1), ln] = body
                tails.append(s_ref[half, pl.ds(t * SW_ + 23 + kw, 8), :])
            pairs = [(max(t, 0), t + T2) for t in range(-2, T2)]
            for i, (p, n) in enumerate(pairs):
                both = jnp.concatenate([tails[p], tails[n]], axis=0).astype(BF16)
                a_ref[kw, h, pl.ds(ABASE + i * TR, TR), ln] = both


def stage_kernel(n_sh, n_sw, feat, lat, gain_in, gbias_in, zyw_in, zyb_in, zbw_in, zbb_in, cw, cb_in,
                 xe_out, ce_out,
                 wv, a_ref, rx, xres, cv, yv, bv, lt, ltf, lv, fb, re, ce, rs, cs, lts, sv, wz,
                 stat_out, stat_in, par, gain, gbias, zyw, zyb, zbw, zbb, cb,
                 ld_sem, w_sem, hs_sem, hr_sem, ls_sem, lr_sem, ss_sem, sr_sem):
    n_dev = n_sh * n_sw
    sh = lax.axis_index("sh")
    sw = lax.axis_index("sw")
    me = sh * n_sw + sw
    has = {"u": sh > 0, "d": sh < n_sh - 1, "l": sw > 0, "r": sw < n_sw - 1}

    ld_feat = pltpu.make_async_copy(feat, fb, ld_sem.at[0])
    ld_lat = pltpu.make_async_copy(lat, lv, ld_sem.at[1])
    ld_lat.start()
    ld_feat.start()
    params = ((gain_in, gain), (gbias_in, gbias), (zyw_in, zyw), (zyb_in, zyb), (zbw_in, zbw), (zbb_in, zbb), (cb_in, cb))
    ld_params = [pltpu.make_async_copy(src, dst, ld_sem.at[2 + i]) for i, (src, dst) in enumerate(params)]
    for ld in ld_params:
        ld.start()

    def ld_weight(n, b, s):
        return pltpu.make_async_copy(cw.at[b, s], wv.at[n], w_sem.at[n])

    for n in range(4):
        ld_weight(n, n // 2, n % 2).start()

    zero_rows = jnp.zeros((FR, 128), BF16)
    for i in (0, HE - 1, HE):
        lt[i] = zero_rows

    def peer_of(j):
        p = lax.rem(me + j, n_dev)
        return p, {"sh": p // n_sw, "sw": lax.rem(p, n_sw)}

    bar = pltpu.get_barrier_semaphore()
    for j in range(1, n_dev):
        pl.semaphore_signal(bar, inc=1, device_id=peer_of(j)[1], device_id_type=MESH)


    def exists(dy, dx):
        c = None
        for cond, use in ((has["u"], dy < 0), (has["d"], dy > 0), (has["l"], dx < 0), (has["r"], dx > 0)):
            if use:
                c = cond if c is None else jnp.logical_and(c, cond)
        return c

    def device(dy, dx):
        return {"sh": sh + dy, "sw": sw + dx}

    def halo_refs(e, dy, dx, src0):
        side = 1 if dx < 0 else 0
        row = HE - 1 if dy < 0 else 0
        if dx == 0:
            src = (src0[0] if dy < 0 else src0[1])
            return src, re.at[e, 1 if dy < 0 else 0]
        col = 0 if dx < 0 else 1
        if dy == 0:
            return cs.at[col], ce.at[e, side, pl.ds(1, H)]
        return cs.at[col, 0 if dy < 0 else H - 1], ce.at[e, side, row]

    def halo_copy(e, d, src0):
        dy, dx = dirs[d]
        src, dst = halo_refs(e, dy, dx, src0)
        return pltpu.make_async_remote_copy(src_ref=src, dst_ref=dst, send_sem=hs_sem.at[e, d],
                                            recv_sem=hr_sem.at[e, d], device_id=device(dy, dx), device_id_type=MESH)

    def lat_copy(d):
        dy, dx = dirs[d]
        if dx == 0:
            src, dst = (lt.at[1], lt.at[HE - 1]) if dy < 0 else (lt.at[H], lt.at[0])
        else:
            col = 0 if dx < 0 else 1
            base = 128 if dx < 0 else 0
            if dy == 0:
                src, dst = lts.at[col], lt.at[HE, pl.ds(base + 16, H * 16)]
            else:
                row = 0 if dy < 0 else H - 1
                there = (HE - 1 if dy < 0 else 0) * 16
                src, dst = lts.at[col, tile(row)], lt.at[HE, pl.ds(base + there, 16)]
        return pltpu.make_async_remote_copy(src_ref=src, dst_ref=dst, send_sem=ls_sem.at[d],
                                            recv_sem=lr_sem.at[d], device_id=device(dy, dx), device_id_type=MESH)

    def for_dirs(make, what, which=ROW_DIRS + COL_DIRS):
        for d in which:
            dy, dx = dirs[d]
            if what == "recv":
                @pl.when(exists(-dy, -dx))
                def _(d=d):
                    make(d).wait_recv()
            else:
                @pl.when(exists(dy, dx))
                def _(d=d):
                    if what == "start":
                        make(d).start()
                    else:
                        make(d).wait_send()

    def stat_copy(n, j):
        p, dev = peer_of(j)
        return pltpu.make_async_remote_copy(src_ref=stat_out.at[n], dst_ref=stat_in.at[n, me], send_sem=ss_sem.at[n, j],
                                            recv_sem=sr_sem.at[n, me], device_id=dev, device_id_type=MESH)

    def send_stats(n, pivot, s1, s2):
        count = float(T * H * W)
        s1 = jnp.sum(s1, axis=0, keepdims=True) * (1.0 / count)
        s2 = jnp.sum(s2, axis=0, keepdims=True) * (1.0 / count)
        mean = pivot + s1
        var = jnp.maximum(s2 - s1 * s1, 0.0)
        rows = [mean[:, :128], mean[:, 128:], var[:, :128], var[:, 128:]]
        packed = jnp.concatenate(rows + [jnp.zeros((4, 128), F32)], axis=0)
        stat_out[n] = packed
        stat_in[n, me] = packed
        for j in range(1, n_dev):
            stat_copy(n, j).start()

    def recv_stats(n, b, s):
        for j in range(1, n_dev):
            p = lax.rem(me + j, n_dev)
            pltpu.make_async_remote_copy(src_ref=stat_out.at[n], dst_ref=stat_in.at[n, p], send_sem=ss_sem.at[n, j],
                                         recv_sem=sr_sem.at[n, p], device_id=peer_of(j)[1], device_id_type=MESH).wait_recv()
        vals = [stat_in[n, i] for i in range(n_dev)]
        total = functools.reduce(jnp.add, vals) * (1.0 / n_dev)
        mean = total[0:2, :]
        dev = functools.reduce(jnp.add, [jnp.square(v[0:2, :] - mean) for v in vals]) * (1.0 / n_dev)
        var = total[2:4, :] + dev
        lane = lax.broadcasted_iota(jnp.int32, (2, 128), 1)
        for gap in (1, 2, 4):
            low = (lane & gap) == 0

            def partner(v):
                return jnp.where(low, pltpu.roll(v, LN - gap, 1), pltpu.roll(v, gap, 1))

            mp, vp = partner(mean), partner(var)
            half_gap = (mean - mp) * 0.5
            var = (var + vp) * 0.5 + half_gap * half_gap
            mean = (mean + mp) * 0.5
        rstd = lax.rsqrt(var + GN_EPSILON)
        mean = jnp.concatenate([mean[0:1], mean[1:2]], axis=1)
        rstd = jnp.concatenate([rstd[0:1], rstd[1:2]], axis=1)
        par[0] = jnp.broadcast_to(mean, (SUB, C))
        par[1] = jnp.broadcast_to(rstd * chan(gain, b, s), (SUB, C))
        par[2] = jnp.broadcast_to(chan(gbias, b, s), (SUB, C))

    def fill_columns(rows):
        for h in rows:
            for side, w in ((0, 0), (1, W - 1)):
                for half in PAIR:
                    v = rx[half, pl.ds((h + 1) * FR + w, TR, stride=W), :]
                    cs[side, h, :, lanes(half)] = v.astype(BF16)

    def main():
        wz[...] = jnp.zeros(wz.shape, BF16)
        ltf[...] = jnp.zeros(ltf.shape, F32)
        ld_lat.wait()

        def turn_row(h, c):
            for t in range(T):
                ltf[pl.ds(h * FR + t * W, W), pl.ds(0, LZ)] = lv[t, h].astype(F32).T
            lt[h + 1] = ltf[pl.ds(pl.multiple_of(h * FR, TR), FR), :].astype(BF16)
            return c

        lax.fori_loop(0, H, turn_row, 0)
        for h in range(H):
            for side, w in ((0, 0), (1, W - 1)):
                lts[side, tile(h), :] = ltf[pl.ds(h * FR + w, TR, stride=W), :].astype(BF16)

        ld_feat.wait()
        pivot0 = fb[0, 0, pl.ds(0, 8), :].astype(F32)[0:1, :]
        pivot8 = jnp.broadcast_to(pivot0, (SUB, C))

        def load_row(h, carry):
            s1, s2 = carry
            for t in range(T):
                x = fb[t, h].astype(F32)
                for half in PAIR:
                    rx[half, pl.ds((h + 1) * FR + t * W, W), :] = x[:, half * LN:half * LN + LN]
                xres[h, pl.ds(t * W, W), :] = x
                for i in TRIO:
                    d = x[i * SUB:i * SUB + SUB] - pivot8
                    s1 = s1 + d
                    s2 = s2 + d * d
            return s1, s2

        zero8 = jnp.zeros((SUB, C), F32)
        s1, s2 = lax.fori_loop(0, H, load_row, (zero8, zero8))
        for t in range(T):
            rs[0, t] = fb[t, 0]
            rs[1, t] = fb[t, H - 1]
        fill_columns(range(H))
        row_src = (rs.at[0], rs.at[1])
        pl.semaphore_wait(bar, n_dev - 1)
        send_stats(0, pivot0, s1, s2)
        for_dirs(lat_copy, "start")
        for_dirs(lambda d: halo_copy(0, d, row_src), "start")
        for ld in ld_params:
            ld.wait()
        for_dirs(lat_copy, "recv")
        for_dirs(lat_copy, "send")

        half_or_zero = {k: jnp.where(v, 0.5, 0.0).astype(F32) for k, v in has.items()}

        def latent_maps(b, s):
            wz[pl.ds(0, LZ), pl.ds(0, C)] = zyw[b, s]
            wz[pl.ds(0, LZ), pl.ds(C, C)] = zbw[b, s]
            biases = (chan(zyb, b, s), chan(zbb, b, s))
            for i in range(HE + 1):
                v = jnp.dot(lt[i], wz[...], preferred_element_type=F32)
                for q, out in ((0, yv), (1, bv)):
                    m = v[:, q * C:q * C + C] + biases[q]
                    if i < HE:
                        f = half_or_zero["u"] if i == 0 else half_or_zero["d"] if i == HE - 1 else 0.5
                        out[i] = m * f
                    else:
                        for seg in range(2 * HE):
                            f = half_or_zero["l" if seg < HE else "r"]
                            if seg % HE == 0:
                                f = f * half_or_zero["u"] * 2.0
                            if seg % HE == HE - 1:
                                f = f * half_or_zero["d"] * 2.0
                            out[i, tile(seg), :] = m[seg * TR:seg * TR + TR] * f

        def activate(x, y, b):
            n = x.shape[0] // 8
            x, y, b = (v.reshape(n, 8, C) for v in (x, y, b))
            hv = ((x - par[0][None]) * par[1][None] + par[2][None]) * y + b
            return (hv * jnp.tanh(hv) + hv).reshape(n * 8, C)

        def halo_rows(e):
            for i, cond in ((0, has["u"]), (1, has["d"])):
                row = 0 if i == 0 else HE - 1
                for t in range(T):
                    v = jnp.where(cond, re[e, i, t].astype(F32), 0.0)
                    for half in PAIR:
                        rx[half, pl.ds(row * FR + t * W, W), :] = v[:, half * LN:half * LN + LN]

        def col_vals(e, side, h):
            cond = has["l"] if side == 0 else has["r"]
            cond = jnp.logical_and(cond, jnp.logical_or(h > 0, has["u"]))
            cond = jnp.logical_and(cond, jnp.logical_or(h < HE - 1, has["d"]))
            return jnp.where(cond, ce[e, side, h].astype(F32), 0.0)

        def activate_rows(n):
            def row(h, c):
                for side in PAIR:
                    k = side * 128 + h * 16
                    v = activate(col_vals(n, side, h), yv[HE, pl.ds(pl.multiple_of(k, TR), TR), :], bv[HE, pl.ds(pl.multiple_of(k, TR), TR), :])
                    for half in PAIR:
                        sv[half, pl.ds(7 + side * 25, T, stride=SW_), :] = v[0:T, half * LN:half * LN + LN]
                for t in range(T):
                    x = jnp.concatenate([rx[half, pl.ds(pl.multiple_of(h * FR, 8) + t * W, W), :] for half in PAIR], axis=1)
                    v = activate(x, yv[h, pl.ds(t * W, W), :], bv[h, pl.ds(t * W, W), :])
                    for half in PAIR:
                        sv[half, pl.ds(t * SW_ + 8, W), :] = v[:, half * LN:half * LN + LN]
                write_operand(a_ref, sv, h)
                return c

            lax.fori_loop(0, HE, row, 0)

        def conv(n, rows, steps):
            def lhs(h, part, tap):
                kt, kh, kw = tap // 9, tap // 3 % 3, tap % 3
                return a_ref[kw, h + kh, pl.ds(kt * 16 + (ABASE if part else 0), NB if part else NA), :]

            for i in steps:
                rhs = jnp.concatenate([wv[n, i * 3 + kw] for kw in TRIO], axis=1)
                for h in rows:
                    cols = [jnp.concatenate([lhs(h, part, i * 3 + kw) for part in PAIR], axis=0) for kw in TRIO]
                    v = lax.dot_general(jnp.concatenate(cols, axis=1), rhs, CONTRACT_LAST, preferred_element_type=F32)
                    if i == 0:
                        cv[h] = v
                    else:
                        cv[h] += v

        def finish(b, s, rows, sums):
            bias = chan(cb, b, s)
            pivot, s1, s2 = sums
            for h in rows:
                for part in PAIR:
                    v = (cv[h, pl.ds(NA if part else 0, NB if part else NA), :] + bias).astype(BF16).astype(F32)
                    nblk = 16 if part == 0 else 8
                    for i in range(T):
                        if part == 0:
                            t, w0 = i, 0
                        else:
                            t, w0 = (i // 2) + (i % 2) * T2, 16
                        blk = v[i * nblk:(i + 1) * nblk]
                        r0 = t * W + w0
                        if s == 1:
                            blk = (blk + xres[h, pl.ds(r0, nblk), :]).astype(BF16).astype(F32)
                            xres[h, pl.ds(r0, nblk), :] = blk
                        for half in PAIR:
                            rx[half, pl.ds((h + 1) * FR + r0, nblk), :] = blk[:, half * LN:half * LN + LN]
                        if h in (0, H - 1):
                            rs[0 if h == 0 else 1, t, pl.ds(w0, nblk), :] = blk.astype(BF16)
                        if s == 1:
                            xe_out[h + 1, t, pl.ds(w0, nblk), :] = blk.astype(BF16)
                        if pivot is None:
                            pivot = blk[0:1, :]
                        for k in range(nblk // 8):
                            d = blk[k * SUB:k * SUB + SUB] - pivot
                            s1 = s1 + d
                            s2 = s2 + d * d
            return pivot, s1, s2

        def block(b, carry):
            for s in PAIR:
                n = b * 2 + s
                latent_maps(b, s)
                for_dirs(lambda d: halo_copy(n, d, row_src), "recv")
                halo_rows(n)
                recv_stats(n, b, s)
                activate_rows(n)
                ld_weight(n, b, s).wait()
                for_dirs(lambda d: halo_copy(n, d, row_src), "send")
                conv(n, EDGE, range(9))
                sums = finish(b, s, EDGE, (None, zero8, zero8))
                fill_columns(EDGE)
                conv(n, INNER, PAIR)
                for_dirs(lambda d: halo_copy(n + 1, d, row_src), "start", ROW_DIRS)
                conv(n, INNER, range(2, 9))
                pivot, s1, s2 = finish(b, s, INNER, sums)
                if s == 0:
                    send_stats(n + 1, pivot, s1, s2)
                else:
                    @pl.when(b == 0)
                    def _():
                        send_stats(n + 1, pivot, s1, s2)
                fill_columns(INNER)
                for_dirs(lambda d: halo_copy(n + 1, d, row_src), "start", COL_DIRS)
            return carry

        lax.fori_loop(0, 2, block, 0)

        for_dirs(lambda d: halo_copy(4, d, row_src), "recv")
        for i, cond in ((0, has["u"]), (1, has["d"])):
            row = 0 if i == 0 else HE - 1
            for t in range(T):
                xe_out[row, t] = jnp.where(cond, re[4, i, t].astype(F32), 0.0).astype(BF16)
        for side in PAIR:
            for h in range(HE):
                ce_out[side, h] = col_vals(4, side, h).astype(BF16)
        for_dirs(lambda d: halo_copy(4, d, row_src), "send")
        for n in range(4):
            for j in range(1, n_dev):
                stat_copy(n, j).wait_send()

    main()


def up_kernel(xe, ce, wu, ub, out, a_ref, sv, o32, part, ob, o_sem):
    def row(h, c):
        for side in PAIR:
            v = ce[side, h].astype(F32)
            for half in PAIR:
                sv[half, pl.ds(7 + side * 25, T, stride=SW_), :] = v[0:T, half * LN:half * LN + LN]
        for t in range(T):
            v = xe[h, t].astype(F32)
            for half in PAIR:
                sv[half, pl.ds(t * SW_ + 8, W), :] = v[:, half * LN:half * LN + LN]
        write_operand(a_ref, sv, h)
        return c

    lax.fori_loop(0, HE, row, 0)

    def out_copy(q, a, hp):
        return pltpu.make_async_copy(ob.at[hp, q, a], out.at[:, 2 * (q * 3 + hp) + a], o_sem.at[hp, q, a])

    def main(*accs):
        for acc in accs:
            pltpu.matmul_pop(acc)

        def row_taps(a):
            return [(1, 1)] if a is None else [(0, a), (2, a + 1)]

        groups = []
        for a in (None, 0, 1):
            for b in (None, 0, 1):
                groups.append((a, b, [(k, l, dh, kw) for k, dh in row_taps(a) for l, kw in row_taps(b)]))
        taps = [(g, tap) for g, grp in enumerate(groups) for tap in grp[2]]

        def push(i):
            k, l, _, _ = taps[i % len(taps)][1]
            for q in PAIR:
                pltpu.matmul_push_rhs(wu[k, l], staging_register=0, mxu_index=q, transpose=True)

        def blocks(q, slot):
            va = pltpu.matmul_pop(accs[q * 6 + slot * 2])
            vb = pltpu.matmul_pop(accs[q * 6 + slot * 2 + 1])
            return va, vb

        push(0)
        for hp in TRIO:
            for i, (g, (k, l, dh, kw)) in enumerate(taps):
                slot = g % 3
                for q in PAIR:
                    pltpu.matmul_acc_lhs(accs[q * 6 + slot * 2], a_ref[kw, q * 3 + hp + dh, pl.ds(32, NA), :], load_staged_rhs=0)
                if hp < 2 or i + 1 < len(taps):
                    push(i + 1)
                for q in PAIR:
                    pltpu.matmul_acc_lhs(accs[q * 6 + slot * 2 + 1], a_ref[kw, q * 3 + hp + dh, pl.ds(ABASE + 32, NB), :])
                if i + 1 < len(taps) and taps[i + 1][0] == g:
                    continue
                a, b, _ = groups[g]
                for q in PAIR:
                    va, vb = blocks(q, slot)
                    for v, sl in ((va, pl.ds(0, NA)), (vb, pl.ds(NA, NB))):
                        if a is None and b is None:
                            part[q, 0, sl, :] = v + ub[...]
                        elif a is None:
                            part[q, 1 + b, sl, :] = v + part[q, 0, sl, :]
                        elif b is None:
                            part[q, 3, sl, :] = v
                    if a is None or b is None:
                        continue
                    va = va + part[q, 1 + b, pl.ds(0, NA), :] + part[q, 3, pl.ds(0, NA), :]
                    vb = vb + part[q, 1 + b, pl.ds(NA, NB), :] + part[q, 3, pl.ds(NA, NB), :]
                    for half in PAIR:
                        ln = slice(half * LN, half * LN + LN)
                        for t in range(T):
                            o32[q, half, pl.ds(t * 2 * W + b, TR, stride=2), :] = va[t * TR:t * TR + TR, ln]
                            kb = (t % T2) * TR + (t // T2) * 8
                            o32[q, half, pl.ds(t * 48 + 32 + b, 8, stride=2), :] = vb[kb:kb + 8, ln]
                    if b == 1:
                        for t in range(T):
                            for half in PAIR:
                                ob[hp, q, a, t, :, lanes(half)] = o32[q, half, pl.ds(t * 2 * W, 2 * W), :].astype(BF16)
                        out_copy(q, a, hp).start()
        for hp in TRIO:
            for q in PAIR:
                for a in PAIR:
                    out_copy(q, a, hp).wait()

    pl.run_scoped(main, *acc_specs())


def solution(mesh):
    n_sh, n_sw = mesh.shape["sh"], mesh.shape["sw"]
    n_dev = n_sh * n_sw
    vmem = pl.BlockSpec(memory_space=pltpu.VMEM)
    hbm = pl.BlockSpec(memory_space=pltpu.HBM)
    dma = pltpu.SemaphoreType.DMA
    vec, mat = pltpu.VMEM((2, 2, C), F32), pltpu.VMEM((2, 2, LZ, C), BF16)

    def local_step(features, latent, gn_gain, gn_bias, zy_weight, zy_bias, zb_weight, zb_bias, conv_weight, conv_bias, up_weight, up_bias):
        feat = features[0].transpose(1, 2, 3, 0)
        lat = latent[0].transpose(1, 2, 0, 3)
        cw = conv_weight.transpose(0, 1, 4, 5, 6, 2, 3).reshape(2, 2, 27, C, C)
        uw = up_weight.transpose(2, 3, 0, 1)
        xe, ce = pl.pallas_call(
            functools.partial(stage_kernel, n_sh, n_sw),
            out_shape=(jax.ShapeDtypeStruct((HE, T, W, C), BF16), jax.ShapeDtypeStruct((2, HE, 16, C), BF16)),
            in_specs=[hbm] * 10,
            out_specs=(vmem, vmem),
            scratch_shapes=[
                pltpu.VMEM((4, 27, C, C), BF16),
                pltpu.VMEM((3, HE, AR, C), BF16),
                pltpu.VMEM((2, HE * FR, 128), F32),
                pltpu.VMEM((H, FR, C), F32),
                pltpu.VMEM((H, FR, C), F32),
                pltpu.VMEM((HE + 1, FR, C), F32),
                pltpu.VMEM((HE + 1, FR, C), F32),
                pltpu.VMEM((HE + 1, FR, 128), BF16),
                pltpu.VMEM((H * FR + 96, 128), F32),
                pltpu.VMEM((T, H, LZ, W), BF16),
                pltpu.VMEM((T, H, W, C), BF16),
                pltpu.VMEM((5, 2, T, W, C), BF16),
                pltpu.VMEM((5, 2, HE, 16, C), BF16),
                pltpu.VMEM((2, T, W, C), BF16),
                pltpu.VMEM((2, H, 16, C), BF16),
                pltpu.VMEM((2, H * 16, 128), BF16),
                pltpu.VMEM((2, T * SW_, 128), F32),
                pltpu.VMEM((128, 2 * C), BF16),
                pltpu.VMEM((4, 8, 128), F32),
                pltpu.VMEM((4, n_dev, 8, 128), F32),
                pltpu.VMEM((3, 8, C), F32),
                vec, vec, mat, vec, mat, vec, vec,
                dma((9,)), dma((4,)), dma((5, 8)), dma((5, 8)), dma((8,)), dma((8,)), dma((4, n_dev)), dma((4, n_dev)),
            ],
            compiler_params=pltpu.CompilerParams(collective_id=0, has_side_effects=True, vmem_limit_bytes=40 << 20),
            name="stages",
        )(*[pltpu.with_memory_space_constraint(v, pltpu.HBM) for v in (feat, lat, gn_gain, gn_bias, zy_weight, zy_bias, zb_weight, zb_bias, cw, conv_bias)])
        out = pl.pallas_call(
            up_kernel,
            out_shape=jax.ShapeDtypeStruct((T, 2 * H, 2 * W, C), BF16),
            in_specs=[vmem] * 4,
            out_specs=hbm,
            scratch_shapes=[
                pltpu.VMEM((3, HE, AR, C), BF16),
                pltpu.VMEM((2, T * SW_, 128), F32),
                pltpu.VMEM((2, 2, T * 2 * W, 128), F32),
                pltpu.VMEM((2, 4, FR, C), F32),
                pltpu.VMEM((3, 2, 2, T, 2 * W, C), BF16),
                dma((3, 2, 2)),
            ],
            compiler_params=pltpu.CompilerParams(vmem_limit_bytes=40 << 20),
            name="upsample",
        )(xe, ce, uw, up_bias.reshape(1, C))
        return out.transpose(3, 0, 1, 2)[None]

    data_spec = P("dp", None, None, "sh", "sw")
    return jax.shard_map(local_step, mesh=mesh, in_specs=(data_spec, data_spec) + (P(),) * 10, out_specs=data_spec, check_vma=False)
```

```python
import functools

import jax
import jax.numpy as jnp
from jax import lax
from jax.experimental import pallas as pl
from jax.experimental.pallas import tpu as pltpu
from jax.sharding import PartitionSpec as P

GN_EPSILON = 1e-6
MESH = pl.DeviceIdType.MESH
F32 = jnp.float32
CONTRACT_LAST = (((1,), (1,)), ((), ()))
BF16 = jnp.bfloat16
T, H, W, C, LZ = 12, 6, 24, 256, 16
HE = H + 2
FR = T * W
NA, NB = T * 16, T * 8
AR = (T + 2) * 16 + (T // 2 + 2) * 16
ABASE = (T + 2) * 16
SW_ = 40
T2 = T // 2
dirs = [(-1, 0), (1, 0), (0, -1), (0, 1), (-1, -1), (-1, 1), (1, -1), (1, 1)]
ROW_DIRS, COL_DIRS = (0, 1, 4, 5, 6, 7), (2, 3)
EDGE, INNER = (0, H - 1), range(1, H - 1)


LN = 128
PAIR, TRIO = range(2), range(3)
GAPS = (1, 2, 4)
TR, SUB = 16, 8


def lanes(half):
    return pl.ds(half * LN, LN)


def tile(i):
    return pl.ds(i * TR, TR)


def chan(ref, b, s):
    return ref[b, pl.ds(s, 1), :]


def acc_specs():
    specs = []
    for q in PAIR:
        for _ in TRIO:
            specs += [pltpu.ACC(q)((NA, C), F32), pltpu.ACC(q)((NB, C), F32)]
    return specs


def write_operand(a_ref, s_ref, h, body_kw=TRIO, tail_kw=TRIO):
    for half in PAIR:
        ln = lanes(half)
        for kw in body_kw:
            for t in range(T):
                body = s_ref[h, half, pl.ds(t * SW_ + 7 + kw, TR), :].astype(BF16)
                a_ref[kw, h, tile(t + 2), ln] = body
                if t == 0:
                    a_ref[kw, h, tile(0), ln] = body
                    a_ref[kw, h, tile(1), ln] = body
        for kw in tail_kw:
            tails = [s_ref[h, half, pl.ds(t * SW_ + 23 + kw, SUB), :] for t in range(T)]
            pairs = [(max(t, 0), t + T2) for t in range(-2, T2)]
            for i, (p, n) in enumerate(pairs):
                both = jnp.concatenate([tails[p], tails[n]], axis=0).astype(BF16)
                a_ref[kw, h, pl.ds(ABASE + i * TR, TR), ln] = both


def stage_kernel(n_sh, n_sw, feat, lat, gain_in, gbias_in, zyw_in, zyb_in, zbw_in, zbb_in, cw, cb_in,
                 aup,
                 wv, a_ref, rx, xres, cv, yv, bv, lt, ltf, lv, fb, re, ce, rs, cs, lts, sv, wz,
                 stat_out, stat_in, par, gain, gbias, zyw, zyb, zbw, zbb, cb,
                 ld_sem, w_sem, hs_sem, hr_sem, ls_sem, lr_sem, ss_sem, sr_sem):
    n_dev = n_sh * n_sw
    sh = lax.axis_index("sh")
    sw = lax.axis_index("sw")
    me = sh * n_sw + sw
    has = {"u": sh > 0, "d": sh < n_sh - 1, "l": sw > 0, "r": sw < n_sw - 1}

    ld_feat = pltpu.make_async_copy(feat, fb, ld_sem.at[0])
    ld_lat = pltpu.make_async_copy(lat, lv, ld_sem.at[1])
    ld_lat.start()
    ld_feat.start()
    params = ((gain_in, gain), (gbias_in, gbias), (zyw_in, zyw), (zyb_in, zyb), (zbw_in, zbw), (zbb_in, zbb), (cb_in, cb))
    ld_params = [pltpu.make_async_copy(src, dst, ld_sem.at[2 + i]) for i, (src, dst) in enumerate(params)]
    for ld in ld_params:
        ld.start()

    def ld_weight(n, b, s):
        return pltpu.make_async_copy(cw.at[b, s], wv.at[n], w_sem.at[n])

    for n in range(4):
        ld_weight(n, n // 2, n % 2).start()

    zero_rows = jnp.zeros((FR, 128), BF16)
    for i in (0, HE - 1, HE):
        lt[i] = zero_rows

    def peer_of(j):
        p = lax.rem(me + j, n_dev)
        return p, {"sh": p // n_sw, "sw": lax.rem(p, n_sw)}

    bar = pltpu.get_barrier_semaphore()
    for j in range(1, n_dev):
        pl.semaphore_signal(bar, inc=1, device_id=peer_of(j)[1], device_id_type=MESH)


    def exists(dy, dx):
        c = None
        for cond, use in ((has["u"], dy < 0), (has["d"], dy > 0), (has["l"], dx < 0), (has["r"], dx > 0)):
            if use:
                c = cond if c is None else jnp.logical_and(c, cond)
        return c

    def device(dy, dx):
        return {"sh": sh + dy, "sw": sw + dx}

    def halo_refs(e, dy, dx, src0):
        side = 1 if dx < 0 else 0
        row = HE - 1 if dy < 0 else 0
        if dx == 0:
            src = (src0[0] if dy < 0 else src0[1])
            return src, re.at[e, 1 if dy < 0 else 0]
        col = 0 if dx < 0 else 1
        if dy == 0:
            return cs.at[col], ce.at[e, side, pl.ds(1, H)]
        return cs.at[col, 0 if dy < 0 else H - 1], ce.at[e, side, row]

    def halo_copy(e, d, src0):
        dy, dx = dirs[d]
        src, dst = halo_refs(e, dy, dx, src0)
        return pltpu.make_async_remote_copy(src_ref=src, dst_ref=dst, send_sem=hs_sem.at[e, d],
                                            recv_sem=hr_sem.at[e, d], device_id=device(dy, dx), device_id_type=MESH)

    def lat_copy(d):
        dy, dx = dirs[d]
        if dx == 0:
            src, dst = (lt.at[1], lt.at[HE - 1]) if dy < 0 else (lt.at[H], lt.at[0])
        else:
            col = 0 if dx < 0 else 1
            base = 128 if dx < 0 else 0
            if dy == 0:
                src, dst = lts.at[col], lt.at[HE, pl.ds(base + 16, H * 16)]
            else:
                row = 0 if dy < 0 else H - 1
                there = (HE - 1 if dy < 0 else 0) * 16
                src, dst = lts.at[col, tile(row)], lt.at[HE, pl.ds(base + there, 16)]
        return pltpu.make_async_remote_copy(src_ref=src, dst_ref=dst, send_sem=ls_sem.at[d],
                                            recv_sem=lr_sem.at[d], device_id=device(dy, dx), device_id_type=MESH)

    def for_dirs(make, what, which=ROW_DIRS + COL_DIRS):
        for d in which:
            dy, dx = dirs[d]
            if what == "recv":
                @pl.when(exists(-dy, -dx))
                def _(d=d):
                    make(d).wait_recv()
            else:
                @pl.when(exists(dy, dx))
                def _(d=d):
                    if what == "start":
                        make(d).start()
                    else:
                        make(d).wait_send()

    def stat_copy(n, j):
        p, dev = peer_of(j)
        return pltpu.make_async_remote_copy(src_ref=stat_out.at[n], dst_ref=stat_in.at[n, me], send_sem=ss_sem.at[n, j],
                                            recv_sem=sr_sem.at[n, me], device_id=dev, device_id_type=MESH)

    lane = lax.broadcasted_iota(jnp.int32, (1, LN), 1) & 7

    def partner(v, gap):
        return jnp.where((lane & gap) == 0, pltpu.roll(v, LN - gap, 1), pltpu.roll(v, gap, 1))

    def stack(v):
        return jnp.concatenate([v[:, :LN], v[:, LN:]], axis=0)

    def send_stats(n, pivot, s1, s2):
        count = 1.0 / (T * H * W)
        s1 = jnp.sum(s1, axis=0, keepdims=True) * count
        s2 = jnp.sum(s2, axis=0, keepdims=True) * count
        mean, var = stack(pivot + s1), stack(jnp.maximum(s2 - s1 * s1, 0.0))
        for gap in GAPS:
            mp, vp = partner(mean, gap), partner(var, gap)
            half_gap = (mean - mp) * 0.5
            var = (var + vp) * 0.5 + half_gap * half_gap
            mean = (mean + mp) * 0.5
        quad = (mean[0:1], mean[1:2], var[0:1], var[1:2])
        row = sum(jnp.where(lane == i, v, 0.0) for i, v in enumerate(quad))
        stat_out[n] = row
        stat_in[n, me] = row
        for j in range(1, n_dev):
            stat_copy(n, j).start()

    def recv_stats(n, b, s):
        for j in range(1, n_dev):
            p, dev = peer_of(j)
            pltpu.make_async_remote_copy(src_ref=stat_out.at[n], dst_ref=stat_in.at[n, p], send_sem=ss_sem.at[n, j],
                                         recv_sem=sr_sem.at[n, p], device_id=dev, device_id_type=MESH).wait_recv()
        vals = [stat_in[n, i] for i in range(n_dev)]
        total = functools.reduce(jnp.add, vals) * (1.0 / n_dev)
        between = functools.reduce(jnp.add, [jnp.square(v - total) for v in vals]) * (1.0 / n_dev)

        def pick(v, i):
            return jnp.where(lane == i, v, 0.0)

        x = jnp.concatenate([pick(total, 0), pick(total, 1), pick(total, 2) + pick(between, 0), pick(total, 3) + pick(between, 1)], axis=0)
        for gap in GAPS:
            x = x + partner(x, gap)
        mean = jnp.concatenate([x[0:1], x[1:2]], axis=1)
        rstd = lax.rsqrt(jnp.concatenate([x[2:3], x[3:4]], axis=1) + GN_EPSILON)
        par[0] = jnp.broadcast_to(mean, (SUB, C))
        par[1] = jnp.broadcast_to(rstd * chan(gain, b, s), (SUB, C))
        par[2] = jnp.broadcast_to(chan(gbias, b, s), (SUB, C))

    def fill_columns(rows):
        for h in rows:
            for side, w in ((0, 0), (1, W - 1)):
                for half in PAIR:
                    v = rx[half, pl.ds((h + 1) * FR + w, TR, stride=W), :]
                    cs[side, h, :, lanes(half)] = v.astype(BF16)

    def main():
        wz[...] = jnp.zeros(wz.shape, BF16)
        ltf[...] = jnp.zeros(ltf.shape, F32)
        ld_lat.wait()

        def turn_row(h, c):
            for t in range(T):
                ltf[pl.ds(h * FR + t * W, W), pl.ds(0, LZ)] = lv[t, h].astype(F32).T
            lt[h + 1] = ltf[pl.ds(pl.multiple_of(h * FR, TR), FR), :].astype(BF16)
            return c

        lax.fori_loop(0, H, turn_row, 0)
        for h in range(H):
            for side, w in ((0, 0), (1, W - 1)):
                lts[side, tile(h), :] = ltf[pl.ds(h * FR + w, TR, stride=W), :].astype(BF16)

        ld_feat.wait()
        pivot0 = fb[0, 0, pl.ds(0, 8), :].astype(F32)[0:1, :]
        pivot8 = jnp.broadcast_to(pivot0, (SUB, C))

        def load_row(h, carry):
            s1, s2 = carry
            for t in range(T):
                x = fb[t, h].astype(F32)
                for half in PAIR:
                    rx[half, pl.ds((h + 1) * FR + t * W, W), :] = x[:, half * LN:half * LN + LN]
                xres[h, pl.ds(t * W, W), :] = x
                for i in TRIO:
                    d = x[i * SUB:i * SUB + SUB] - pivot8
                    s1 = s1 + d
                    s2 = s2 + d * d
            return s1, s2

        zero8 = jnp.zeros((SUB, C), F32)
        s1, s2 = lax.fori_loop(0, H, load_row, (zero8, zero8))
        for t in range(T):
            rs[0, t] = fb[t, 0]
            rs[1, t] = fb[t, H - 1]
        fill_columns(range(H))
        row_src = (rs.at[0], rs.at[1])
        pl.semaphore_wait(bar, n_dev - 1)
        send_stats(0, pivot0, s1, s2)
        for_dirs(lat_copy, "start")
        for_dirs(lambda d: halo_copy(0, d, row_src), "start")
        for ld in ld_params:
            ld.wait()
        for_dirs(lat_copy, "recv")
        for_dirs(lat_copy, "send")

        half_or_zero = {k: jnp.where(v, 0.5, 0.0).astype(F32) for k, v in has.items()}

        def latent_maps(b, s):
            wz[pl.ds(0, LZ), pl.ds(0, C)] = zyw[b, s]
            wz[pl.ds(0, LZ), pl.ds(C, C)] = zbw[b, s]
            biases = (chan(zyb, b, s), chan(zbb, b, s))
            for i in range(HE + 1):
                v = jnp.dot(lt[i], wz[...], preferred_element_type=F32)
                for q, out in ((0, yv), (1, bv)):
                    m = v[:, q * C:q * C + C] + biases[q]
                    if i < HE:
                        f = half_or_zero["u"] if i == 0 else half_or_zero["d"] if i == HE - 1 else 0.5
                        out[i] = m * f
                    else:
                        for seg in range(2 * HE):
                            f = half_or_zero["l" if seg < HE else "r"]
                            if seg % HE == 0:
                                f = f * half_or_zero["u"] * 2.0
                            if seg % HE == HE - 1:
                                f = f * half_or_zero["d"] * 2.0
                            out[i, tile(seg), :] = m[seg * TR:seg * TR + TR] * f

        def activate(x, y, b):
            n = x.shape[0] // 8
            x, y, b = (v.reshape(n, 8, C) for v in (x, y, b))
            hv = ((x - par[0][None]) * par[1][None] + par[2][None]) * y + b
            return (hv * jnp.tanh(hv) + hv).reshape(n * 8, C)

        def halo_rows(e):
            for i, cond in ((0, has["u"]), (1, has["d"])):
                row = 0 if i == 0 else HE - 1
                for t in range(T):
                    v = jnp.where(cond, re[e, i, t].astype(F32), 0.0)
                    for half in PAIR:
                        rx[half, pl.ds(row * FR + t * W, W), :] = v[:, half * LN:half * LN + LN]

        def col_vals(e, side, h):
            cond = has["l"] if side == 0 else has["r"]
            cond = jnp.logical_and(cond, jnp.logical_or(h > 0, has["u"]))
            cond = jnp.logical_and(cond, jnp.logical_or(h < HE - 1, has["d"]))
            return jnp.where(cond, ce[e, side, h].astype(F32), 0.0)

        def put_column(h, side, v):
            for half in PAIR:
                sv[h, half, pl.ds(7 + side * 25, T, stride=SW_), :] = v[0:T, half * LN:half * LN + LN]

        def own_rows(h, t, half):
            return rx[half, pl.ds(pl.multiple_of(h * FR, SUB) + t * W, W), :]

        def activate_rows(n):
            def row(h, c):
                for side in PAIR:
                    at = pl.ds(pl.multiple_of(side * LN + h * TR, TR), TR)
                    put_column(h, side, activate(col_vals(n, side, h), yv[HE, at, :], bv[HE, at, :]))
                for t in range(T):
                    x = jnp.concatenate([own_rows(h, t, half) for half in PAIR], axis=1)
                    v = activate(x, yv[h, pl.ds(t * W, W), :], bv[h, pl.ds(t * W, W), :])
                    for half in PAIR:
                        sv[h, half, pl.ds(t * SW_ + 8, W), :] = v[:, half * LN:half * LN + LN]
                write_operand(a_ref, sv, h)
                return c

            lax.fori_loop(0, HE, row, 0)

        def plain_row(h, c):
            for t in range(T):
                for half in PAIR:
                    sv[h, half, pl.ds(t * SW_ + 8, W), :] = own_rows(h, t, half)
            write_operand(aup, sv, h)
            return c

        def plain_edges(h, c):
            for side in PAIR:
                put_column(h, side, col_vals(4, side, h))
            write_operand(aup, sv, h, (0,), (2,))
            return c

        def conv(n, rows, steps):
            def lhs(h, part, tap):
                kt, kh, kw = tap // 9, tap // 3 % 3, tap % 3
                return a_ref[kw, h + kh, pl.ds(kt * 16 + (ABASE if part else 0), NB if part else NA), :]

            for i in steps:
                rhs = jnp.concatenate([wv[n, i * 3 + kw] for kw in TRIO], axis=1)
                for h in rows:
                    cols = [jnp.concatenate([lhs(h, part, i * 3 + kw) for part in PAIR], axis=0) for kw in TRIO]
                    v = lax.dot_general(jnp.concatenate(cols, axis=1), rhs, CONTRACT_LAST, preferred_element_type=F32)
                    if i == 0:
                        cv[h] = v
                    else:
                        cv[h] += v

        def finish(b, s, rows, sums):
            bias = chan(cb, b, s)
            pivot, s1, s2 = sums
            for h in rows:
                for part in PAIR:
                    v = (cv[h, pl.ds(NA if part else 0, NB if part else NA), :] + bias).astype(BF16).astype(F32)
                    nblk = 16 if part == 0 else 8
                    for i in range(T):
                        if part == 0:
                            t, w0 = i, 0
                        else:
                            t, w0 = (i // 2) + (i % 2) * T2, 16
                        blk = v[i * nblk:(i + 1) * nblk]
                        r0 = t * W + w0
                        if s == 1:
                            blk = (blk + xres[h, pl.ds(r0, nblk), :]).astype(BF16).astype(F32)
                            xres[h, pl.ds(r0, nblk), :] = blk
                        for half in PAIR:
                            rx[half, pl.ds((h + 1) * FR + r0, nblk), :] = blk[:, half * LN:half * LN + LN]
                        if h in (0, H - 1):
                            rs[0 if h == 0 else 1, t, pl.ds(w0, nblk), :] = blk.astype(BF16)
                        if pivot is None:
                            pivot = blk[0:1, :]
                        for k in range(nblk // 8):
                            d = blk[k * SUB:k * SUB + SUB] - pivot
                            s1 = s1 + d
                            s2 = s2 + d * d
            return pivot, s1, s2

        def block(b, carry):
            for s in PAIR:
                n = b * 2 + s
                latent_maps(b, s)
                for_dirs(lambda d: halo_copy(n, d, row_src), "recv")
                halo_rows(n)
                recv_stats(n, b, s)
                activate_rows(n)
                ld_weight(n, b, s).wait()
                for_dirs(lambda d: halo_copy(n, d, row_src), "send")
                conv(n, EDGE, range(9))
                sums = finish(b, s, EDGE, (None, zero8, zero8))
                fill_columns(EDGE)
                conv(n, INNER, PAIR)
                for_dirs(lambda d: halo_copy(n + 1, d, row_src), "start", ROW_DIRS)
                conv(n, INNER, range(2, 9))
                pivot, s1, s2 = finish(b, s, INNER, sums)
                if s == 0:
                    send_stats(n + 1, pivot, s1, s2)
                else:
                    @pl.when(b == 0)
                    def _():
                        send_stats(n + 1, pivot, s1, s2)
                fill_columns(INNER)
                for_dirs(lambda d: halo_copy(n + 1, d, row_src), "start", COL_DIRS)
            return carry

        lax.fori_loop(0, 2, block, 0)

        lax.fori_loop(1, HE - 1, plain_row, 0)
        for_dirs(lambda d: halo_copy(4, d, row_src), "recv", ROW_DIRS)
        halo_rows(4)
        for h in (0, HE - 1):
            plain_row(h, 0)
        for_dirs(lambda d: halo_copy(4, d, row_src), "recv", COL_DIRS)
        lax.fori_loop(0, HE, plain_edges, 0)
        for_dirs(lambda d: halo_copy(4, d, row_src), "send")
        for n in range(4):
            for j in range(1, n_dev):
                stat_copy(n, j).wait_send()

    main()


def up_kernel(a_ref, wu, ub, out, o32, part, ob, o_sem):
    def out_copy(q, a, hp):
        return pltpu.make_async_copy(ob.at[hp, q, a], out.at[:, 2 * (q * 3 + hp) + a], o_sem.at[hp, q, a])

    def main(*accs):
        for acc in accs:
            pltpu.matmul_pop(acc)

        def row_taps(a):
            return [(1, 1)] if a is None else [(0, a), (2, a + 1)]

        groups = []
        for a in (None, 0, 1):
            for b in (None, 0, 1):
                groups.append((a, b, [(k, l, dh, kw) for k, dh in row_taps(a) for l, kw in row_taps(b)]))
        taps = [(g, tap) for g, grp in enumerate(groups) for tap in grp[2]]

        def push(i):
            k, l, _, _ = taps[i % len(taps)][1]
            for q in PAIR:
                pltpu.matmul_push_rhs(wu[k, l], staging_register=0, mxu_index=q, transpose=True)

        def blocks(q, slot):
            va = pltpu.matmul_pop(accs[q * 6 + slot * 2])
            vb = pltpu.matmul_pop(accs[q * 6 + slot * 2 + 1])
            return va, vb

        push(0)
        for hp in TRIO:
            for i, (g, (k, l, dh, kw)) in enumerate(taps):
                slot = g % 3
                for q in PAIR:
                    pltpu.matmul_acc_lhs(accs[q * 6 + slot * 2], a_ref[kw, q * 3 + hp + dh, pl.ds(32, NA), :], load_staged_rhs=0)
                if hp < 2 or i + 1 < len(taps):
                    push(i + 1)
                for q in PAIR:
                    pltpu.matmul_acc_lhs(accs[q * 6 + slot * 2 + 1], a_ref[kw, q * 3 + hp + dh, pl.ds(ABASE + 32, NB), :])
                if i + 1 < len(taps) and taps[i + 1][0] == g:
                    continue
                a, b, _ = groups[g]
                for q in PAIR:
                    va, vb = blocks(q, slot)
                    for v, sl in ((va, pl.ds(0, NA)), (vb, pl.ds(NA, NB))):
                        if a is None and b is None:
                            part[q, 0, sl, :] = v + ub[...]
                        elif a is None:
                            part[q, 1 + b, sl, :] = v + part[q, 0, sl, :]
                        elif b is None:
                            part[q, 3, sl, :] = v
                    if a is None or b is None:
                        continue
                    va = va + part[q, 1 + b, pl.ds(0, NA), :] + part[q, 3, pl.ds(0, NA), :]
                    vb = vb + part[q, 1 + b, pl.ds(NA, NB), :] + part[q, 3, pl.ds(NA, NB), :]
                    for half in PAIR:
                        ln = slice(half * LN, half * LN + LN)
                        for t in range(T):
                            o32[q, half, pl.ds(t * 2 * W + b, TR, stride=2), :] = va[t * TR:t * TR + TR, ln]
                            kb = (t % T2) * TR + (t // T2) * 8
                            o32[q, half, pl.ds(t * 48 + 32 + b, 8, stride=2), :] = vb[kb:kb + 8, ln]
                    if b == 1:
                        for t in range(T):
                            for half in PAIR:
                                ob[hp, q, a, t, :, lanes(half)] = o32[q, half, pl.ds(t * 2 * W, 2 * W), :].astype(BF16)
                        out_copy(q, a, hp).start()
        for hp in TRIO:
            for q in PAIR:
                for a in PAIR:
                    out_copy(q, a, hp).wait()

    pl.run_scoped(main, *acc_specs())


def solution(mesh):
    n_sh, n_sw = mesh.shape["sh"], mesh.shape["sw"]
    n_dev = n_sh * n_sw
    vmem = pl.BlockSpec(memory_space=pltpu.VMEM)
    hbm = pl.BlockSpec(memory_space=pltpu.HBM)
    dma = pltpu.SemaphoreType.DMA
    vec, mat = pltpu.VMEM((2, 2, C), F32), pltpu.VMEM((2, 2, LZ, C), BF16)

    def local_step(features, latent, gn_gain, gn_bias, zy_weight, zy_bias, zb_weight, zb_bias, conv_weight, conv_bias, up_weight, up_bias):
        feat = features[0].transpose(1, 2, 3, 0)
        lat = latent[0].transpose(1, 2, 0, 3)
        cw = conv_weight.transpose(0, 1, 4, 5, 6, 2, 3).reshape(2, 2, 27, C, C)
        uw = up_weight.transpose(2, 3, 0, 1)
        aup = pl.pallas_call(
            functools.partial(stage_kernel, n_sh, n_sw),
            out_shape=jax.ShapeDtypeStruct((3, HE, AR, C), BF16),
            in_specs=[hbm] * 10,
            out_specs=vmem,
            scratch_shapes=[
                pltpu.VMEM((4, 27, C, C), BF16),
                pltpu.VMEM((3, HE, AR, C), BF16),
                pltpu.VMEM((2, HE * FR, 128), F32),
                pltpu.VMEM((H, FR, C), F32),
                pltpu.VMEM((H, FR, C), F32),
                pltpu.VMEM((HE + 1, FR, C), F32),
                pltpu.VMEM((HE + 1, FR, C), F32),
                pltpu.VMEM((HE + 1, FR, 128), BF16),
                pltpu.VMEM((H * FR + 96, 128), F32),
                pltpu.VMEM((T, H, LZ, W), BF16),
                pltpu.VMEM((T, H, W, C), BF16),
                pltpu.VMEM((5, 2, T, W, C), BF16),
                pltpu.VMEM((5, 2, HE, 16, C), BF16),
                pltpu.VMEM((2, T, W, C), BF16),
                pltpu.VMEM((2, H, 16, C), BF16),
                pltpu.VMEM((2, H * 16, 128), BF16),
                pltpu.VMEM((HE, 2, T * SW_, LN), F32),
                pltpu.VMEM((LN, 2 * C), BF16),
                pltpu.VMEM((4, 1, LN), F32),
                pltpu.VMEM((4, n_dev, 1, LN), F32),
                pltpu.VMEM((3, 8, C), F32),
                vec, vec, mat, vec, mat, vec, vec,
                dma((9,)), dma((4,)), dma((5, 8)), dma((5, 8)), dma((8,)), dma((8,)), dma((4, n_dev)), dma((4, n_dev)),
            ],
            compiler_params=pltpu.CompilerParams(collective_id=0, has_side_effects=True, vmem_limit_bytes=42 << 20),
            name="stages",
        )(*[pltpu.with_memory_space_constraint(v, pltpu.HBM) for v in (feat, lat, gn_gain, gn_bias, zy_weight, zy_bias, zb_weight, zb_bias, cw, conv_bias)])
        out = pl.pallas_call(
            up_kernel,
            out_shape=jax.ShapeDtypeStruct((T, 2 * H, 2 * W, C), BF16),
            in_specs=[vmem] * 3,
            out_specs=hbm,
            scratch_shapes=[
                pltpu.VMEM((2, 2, T * 2 * W, LN), F32),
                pltpu.VMEM((2, 4, FR, C), F32),
                pltpu.VMEM((3, 2, 2, T, 2 * W, C), BF16),
                dma((3, 2, 2)),
            ],
            compiler_params=pltpu.CompilerParams(vmem_limit_bytes=24 << 20),
            name="upsample",
        )(aup, uw, up_bias.reshape(1, C))
        return out.transpose(3, 0, 1, 2)[None]

    data_spec = P("dp", None, None, "sh", "sw")
    return jax.shard_map(local_step, mesh=mesh, in_specs=(data_spec, data_spec) + (P(),) * 10, out_specs=data_spec, check_vma=False)
```

```python
import functools

import jax
import jax.numpy as jnp
from jax import lax
from jax.experimental import pallas as pl
from jax.experimental.pallas import tpu as pltpu
from jax.sharding import PartitionSpec as P

GN_EPSILON = 1e-6
MESH = pl.DeviceIdType.MESH
F32 = jnp.float32
CONTRACT_LAST = (((1,), (1,)), ((), ()))
BF16 = jnp.bfloat16
T, H, W, C, LZ = 12, 6, 24, 256, 16
HE = H + 2
FR = T * W
NA, NB = T * 16, T * 8
AR = (T + 2) * 16 + (T // 2 + 2) * 16
ABASE = (T + 2) * 16
SW_ = 40
T2 = T // 2
dirs = [(-1, 0), (1, 0), (0, -1), (0, 1), (-1, -1), (-1, 1), (1, -1), (1, 1)]
ROW_DIRS, COL_DIRS = (0, 1, 4, 5, 6, 7), (2, 3)
EDGE, INNER = (0, H - 1), range(1, H - 1)


LN = 128
PAIR, TRIO = range(2), range(3)
GAPS = (1, 2, 4)
NTAP, EARLY = 27, 6
TR, SUB = 16, 8


def lanes(half):
    return pl.ds(half * LN, LN)


def tile(i):
    return pl.ds(i * TR, TR)


def chan(ref, b, s):
    return ref[b, pl.ds(s, 1), :]


def acc_specs():
    specs = []
    for q in PAIR:
        for _ in TRIO:
            specs += [pltpu.ACC(q)((NA, C), F32), pltpu.ACC(q)((NB, C), F32)]
    return specs


def write_operand(a_ref, s_ref, h, body_kw=TRIO, tail_kw=TRIO):
    for half in PAIR:
        ln = lanes(half)
        for kw in body_kw:
            for t in range(T):
                body = s_ref[h, half, pl.ds(t * SW_ + 7 + kw, TR), :].astype(BF16)
                a_ref[kw, h, tile(t + 2), ln] = body
                if t == 0:
                    a_ref[kw, h, tile(0), ln] = body
                    a_ref[kw, h, tile(1), ln] = body
        for kw in tail_kw:
            tails = [s_ref[h, half, pl.ds(t * SW_ + 23 + kw, SUB), :] for t in range(T)]
            pairs = [(max(t, 0), t + T2) for t in range(-2, T2)]
            for i, (p, n) in enumerate(pairs):
                both = jnp.concatenate([tails[p], tails[n]], axis=0).astype(BF16)
                a_ref[kw, h, pl.ds(ABASE + i * TR, TR), ln] = both


def stage_kernel(n_sh, n_sw, feat, lat, gain_in, gbias_in, zyw_in, zyb_in, zbw_in, zbb_in, cw, cb_in,
                 aup,
                 wv, a_ref, rx, xres, cv, yv, bv, lt, ltf, lv, fb, re, ce, rs, cs, lts, sv, wz,
                 stat_out, stat_in, par, gain, gbias, zyw, zyb, zbw, zbb, cb,
                 ld_sem, w_sem, hs_sem, hr_sem, ls_sem, lr_sem, ss_sem, sr_sem):
    n_dev = n_sh * n_sw
    sh = lax.axis_index("sh")
    sw = lax.axis_index("sw")
    me = sh * n_sw + sw
    has = {"u": sh > 0, "d": sh < n_sh - 1, "l": sw > 0, "r": sw < n_sw - 1}

    ld_feat = pltpu.make_async_copy(feat, fb, ld_sem.at[0])
    ld_lat = pltpu.make_async_copy(lat, lv, ld_sem.at[1])
    ld_lat.start()
    ld_feat.start()
    params = ((gain_in, gain), (gbias_in, gbias), (zyw_in, zyw), (zyb_in, zyb), (zbw_in, zbw), (zbb_in, zbb), (cb_in, cb))
    ld_params = [pltpu.make_async_copy(src, dst, ld_sem.at[2 + i]) for i, (src, dst) in enumerate(params)]
    for ld in ld_params:
        ld.start()

    def ld_weight(n, b, s):
        return pltpu.make_async_copy(cw.at[b, s], wv.at[n], w_sem.at[n])

    for n in range(4):
        ld_weight(n, n // 2, n % 2).start()

    zero_rows = jnp.zeros((FR, 128), BF16)
    for i in (0, HE - 1, HE):
        lt[i] = zero_rows

    def peer_of(j):
        p = lax.rem(me + j, n_dev)
        return p, {"sh": p // n_sw, "sw": lax.rem(p, n_sw)}

    bar = pltpu.get_barrier_semaphore()
    for j in range(1, n_dev):
        pl.semaphore_signal(bar, inc=1, device_id=peer_of(j)[1], device_id_type=MESH)


    def exists(dy, dx):
        c = None
        for cond, use in ((has["u"], dy < 0), (has["d"], dy > 0), (has["l"], dx < 0), (has["r"], dx > 0)):
            if use:
                c = cond if c is None else jnp.logical_and(c, cond)
        return c

    def device(dy, dx):
        return {"sh": sh + dy, "sw": sw + dx}

    def halo_refs(e, dy, dx, src0):
        side = 1 if dx < 0 else 0
        row = HE - 1 if dy < 0 else 0
        if dx == 0:
            src = (src0[0] if dy < 0 else src0[1])
            return src, re.at[e, 1 if dy < 0 else 0]
        col = 0 if dx < 0 else 1
        if dy == 0:
            return cs.at[col], ce.at[e, side, pl.ds(1, H)]
        return cs.at[col, 0 if dy < 0 else H - 1], ce.at[e, side, row]

    def halo_copy(e, d, src0):
        dy, dx = dirs[d]
        src, dst = halo_refs(e, dy, dx, src0)
        return pltpu.make_async_remote_copy(src_ref=src, dst_ref=dst, send_sem=hs_sem.at[e, d],
                                            recv_sem=hr_sem.at[e, d], device_id=device(dy, dx), device_id_type=MESH)

    def lat_copy(d):
        dy, dx = dirs[d]
        if dx == 0:
            src, dst = (lt.at[1], lt.at[HE - 1]) if dy < 0 else (lt.at[H], lt.at[0])
        else:
            col = 0 if dx < 0 else 1
            base = 128 if dx < 0 else 0
            if dy == 0:
                src, dst = lts.at[col], lt.at[HE, pl.ds(base + 16, H * 16)]
            else:
                row = 0 if dy < 0 else H - 1
                there = (HE - 1 if dy < 0 else 0) * 16
                src, dst = lts.at[col, tile(row)], lt.at[HE, pl.ds(base + there, 16)]
        return pltpu.make_async_remote_copy(src_ref=src, dst_ref=dst, send_sem=ls_sem.at[d],
                                            recv_sem=lr_sem.at[d], device_id=device(dy, dx), device_id_type=MESH)

    def for_dirs(make, what, which=ROW_DIRS + COL_DIRS):
        for d in which:
            dy, dx = dirs[d]
            if what == "recv":
                @pl.when(exists(-dy, -dx))
                def _(d=d):
                    make(d).wait_recv()
            else:
                @pl.when(exists(dy, dx))
                def _(d=d):
                    if what == "start":
                        make(d).start()
                    else:
                        make(d).wait_send()

    def stat_copy(n, j):
        p, dev = peer_of(j)
        return pltpu.make_async_remote_copy(src_ref=stat_out.at[n], dst_ref=stat_in.at[n, me], send_sem=ss_sem.at[n, j],
                                            recv_sem=sr_sem.at[n, me], device_id=dev, device_id_type=MESH)

    lane = lax.broadcasted_iota(jnp.int32, (1, LN), 1) & 7

    def partner(v, gap):
        return jnp.where((lane & gap) == 0, pltpu.roll(v, LN - gap, 1), pltpu.roll(v, gap, 1))

    def stack(v):
        return jnp.concatenate([v[:, :LN], v[:, LN:]], axis=0)

    def send_stats(n, pivot, s1, s2):
        count = 1.0 / (T * H * W)
        s1 = jnp.sum(s1, axis=0, keepdims=True) * count
        s2 = jnp.sum(s2, axis=0, keepdims=True) * count
        mean, var = stack(pivot + s1), stack(jnp.maximum(s2 - s1 * s1, 0.0))
        for gap in GAPS:
            mp, vp = partner(mean, gap), partner(var, gap)
            half_gap = (mean - mp) * 0.5
            var = (var + vp) * 0.5 + half_gap * half_gap
            mean = (mean + mp) * 0.5
        quad = (mean[0:1], mean[1:2], var[0:1], var[1:2])
        row = sum(jnp.where(lane == i, v, 0.0) for i, v in enumerate(quad))
        stat_out[n] = row
        stat_in[n, me] = row
        for j in range(1, n_dev):
            stat_copy(n, j).start()

    def recv_stats(n, b, s):
        for j in range(1, n_dev):
            p, dev = peer_of(j)
            pltpu.make_async_remote_copy(src_ref=stat_out.at[n], dst_ref=stat_in.at[n, p], send_sem=ss_sem.at[n, j],
                                         recv_sem=sr_sem.at[n, p], device_id=dev, device_id_type=MESH).wait_recv()
        vals = [stat_in[n, i] for i in range(n_dev)]
        total = functools.reduce(jnp.add, vals) * (1.0 / n_dev)
        between = functools.reduce(jnp.add, [jnp.square(v - total) for v in vals]) * (1.0 / n_dev)

        def pick(v, i):
            return jnp.where(lane == i, v, 0.0)

        x = jnp.concatenate([pick(total, 0), pick(total, 1), pick(total, 2) + pick(between, 0), pick(total, 3) + pick(between, 1)], axis=0)
        for gap in GAPS:
            x = x + partner(x, gap)
        mean = jnp.concatenate([x[0:1], x[1:2]], axis=1)
        rstd = lax.rsqrt(jnp.concatenate([x[2:3], x[3:4]], axis=1) + GN_EPSILON)
        par[0] = jnp.broadcast_to(mean, (SUB, C))
        par[1] = jnp.broadcast_to(rstd * chan(gain, b, s), (SUB, C))
        par[2] = jnp.broadcast_to(chan(gbias, b, s), (SUB, C))

    def fill_columns(rows):
        for h in rows:
            for side, w in ((0, 0), (1, W - 1)):
                for half in PAIR:
                    v = rx[half, pl.ds((h + 1) * FR + w, TR, stride=W), :]
                    cs[side, h, :, lanes(half)] = v.astype(BF16)

    def main():
        wz[...] = jnp.zeros(wz.shape, BF16)
        ltf[...] = jnp.zeros(ltf.shape, F32)
        ld_lat.wait()

        def turn_row(h, c):
            for t in range(T):
                ltf[pl.ds(h * FR + t * W, W), pl.ds(0, LZ)] = lv[t, h].astype(F32).T
            lt[h + 1] = ltf[pl.ds(pl.multiple_of(h * FR, TR), FR), :].astype(BF16)
            return c

        lax.fori_loop(0, H, turn_row, 0)
        for h in range(H):
            for side, w in ((0, 0), (1, W - 1)):
                lts[side, tile(h), :] = ltf[pl.ds(h * FR + w, TR, stride=W), :].astype(BF16)

        ld_feat.wait()
        pivot0 = fb[0, 0, pl.ds(0, 8), :].astype(F32)[0:1, :]
        pivot8 = jnp.broadcast_to(pivot0, (SUB, C))

        def load_row(h, carry):
            s1, s2 = carry
            for t in range(T):
                x = fb[t, h].astype(F32)
                for half in PAIR:
                    rx[half, pl.ds((h + 1) * FR + t * W, W), :] = x[:, half * LN:half * LN + LN]
                xres[h, pl.ds(t * W, W), :] = x
                for i in TRIO:
                    d = x[i * SUB:i * SUB + SUB] - pivot8
                    s1 = s1 + d
                    s2 = s2 + d * d
            return s1, s2

        zero8 = jnp.zeros((SUB, C), F32)
        s1, s2 = lax.fori_loop(0, H, load_row, (zero8, zero8))
        for t in range(T):
            rs[0, t] = fb[t, 0]
            rs[1, t] = fb[t, H - 1]
        fill_columns(range(H))
        row_src = (rs.at[0], rs.at[1])
        pl.semaphore_wait(bar, n_dev - 1)
        send_stats(0, pivot0, s1, s2)
        for_dirs(lat_copy, "start")
        for_dirs(lambda d: halo_copy(0, d, row_src), "start")
        for ld in ld_params:
            ld.wait()
        for_dirs(lat_copy, "recv")
        for_dirs(lat_copy, "send")

        half_or_zero = {k: jnp.where(v, 0.5, 0.0).astype(F32) for k, v in has.items()}

        def latent_maps(b, s):
            wz[pl.ds(0, LZ), pl.ds(0, C)] = zyw[b, s]
            wz[pl.ds(0, LZ), pl.ds(C, C)] = zbw[b, s]
            biases = (chan(zyb, b, s), chan(zbb, b, s))
            for i in range(HE + 1):
                v = jnp.dot(lt[i], wz[...], preferred_element_type=F32)
                for q, out in ((0, yv), (1, bv)):
                    m = v[:, q * C:q * C + C] + biases[q]
                    if i < HE:
                        f = half_or_zero["u"] if i == 0 else half_or_zero["d"] if i == HE - 1 else 0.5
                        out[i] = m * f
                    else:
                        for seg in range(2 * HE):
                            f = half_or_zero["l" if seg < HE else "r"]
                            if seg % HE == 0:
                                f = f * half_or_zero["u"] * 2.0
                            if seg % HE == HE - 1:
                                f = f * half_or_zero["d"] * 2.0
                            out[i, tile(seg), :] = m[seg * TR:seg * TR + TR] * f

        def activate(x, y, b):
            n = x.shape[0] // 8
            x, y, b = (v.reshape(n, 8, C) for v in (x, y, b))
            hv = ((x - par[0][None]) * par[1][None] + par[2][None]) * y + b
            return (hv * jnp.tanh(hv) + hv).reshape(n * 8, C)

        def halo_rows(e):
            for i, cond in ((0, has["u"]), (1, has["d"])):
                row = 0 if i == 0 else HE - 1
                for t in range(T):
                    v = jnp.where(cond, re[e, i, t].astype(F32), 0.0)
                    for half in PAIR:
                        rx[half, pl.ds(row * FR + t * W, W), :] = v[:, half * LN:half * LN + LN]

        def col_vals(e, side, h):
            cond = has["l"] if side == 0 else has["r"]
            cond = jnp.logical_and(cond, jnp.logical_or(jnp.int32(h) > 0, has["u"]))
            cond = jnp.logical_and(cond, jnp.logical_or(jnp.int32(h) < HE - 1, has["d"]))
            return jnp.where(cond, ce[e, side, h].astype(F32), 0.0)

        def put_column(h, side, v):
            for half in PAIR:
                sv[h, half, pl.ds(7 + side * 25, T, stride=SW_), :] = v[0:T, half * LN:half * LN + LN]

        def own_rows(h, t, half):
            return rx[half, pl.ds(pl.multiple_of(h * FR, SUB) + t * W, W), :]

        def activate_row(n, h):
            for side in PAIR:
                at = pl.ds(pl.multiple_of(side * LN + h * TR, TR), TR)
                put_column(h, side, activate(col_vals(n, side, h), yv[HE, at, :], bv[HE, at, :]))
            for t in range(T):
                x = jnp.concatenate([own_rows(h, t, half) for half in PAIR], axis=1)
                v = activate(x, yv[h, pl.ds(t * W, W), :], bv[h, pl.ds(t * W, W), :])
                for half in PAIR:
                    sv[h, half, pl.ds(t * SW_ + 8, W), :] = v[:, half * LN:half * LN + LN]
            write_operand(a_ref, sv, h)

        def plain_row(h, c):
            for t in range(T):
                for half in PAIR:
                    sv[h, half, pl.ds(t * SW_ + 8, W), :] = own_rows(h, t, half)
            write_operand(aup, sv, h)
            return c

        def plain_edges(h, c):
            for side in PAIR:
                put_column(h, side, col_vals(4, side, h))
            write_operand(aup, sv, h, (0,), (2,))
            return c

        def conv(n, rows, taps):
            def lhs(h, part, tap):
                kt, kh, kw = tap // 9, tap // 3 % 3, tap % 3
                return a_ref[kw, h + kh, pl.ds(kt * 16 + (ABASE if part else 0), NB if part else NA), :]

            for h in rows:
                rhs = jnp.concatenate([wv[n, i] for i in taps], axis=1)
                cols = [jnp.concatenate([lhs(h, part, i) for part in PAIR], axis=0) for i in taps]
                v = lax.dot_general(jnp.concatenate(cols, axis=1), rhs, CONTRACT_LAST, preferred_element_type=F32)
                if taps[0] == 0:
                    cv[h] = v
                else:
                    cv[h] += v

        def finish(b, s, rows, sums):
            bias = chan(cb, b, s)
            second = s == 1
            pivot, s1, s2 = sums
            for h in rows:
                for part in PAIR:
                    v = (cv[h, pl.ds(NA if part else 0, NB if part else NA), :] + bias).astype(BF16).astype(F32)
                    nblk = 16 if part == 0 else 8
                    for i in range(T):
                        if part == 0:
                            t, w0 = i, 0
                        else:
                            t, w0 = (i // 2) + (i % 2) * T2, 16
                        blk = v[i * nblk:(i + 1) * nblk]
                        r0 = t * W + w0
                        res = xres[h, pl.ds(r0, nblk), :]
                        blk = (blk + jnp.where(second, res, 0.0)).astype(BF16).astype(F32)
                        xres[h, pl.ds(r0, nblk), :] = jnp.where(second, blk, res)
                        for half in PAIR:
                            rx[half, pl.ds((h + 1) * FR + r0, nblk), :] = blk[:, half * LN:half * LN + LN]
                        if h in (0, H - 1):
                            rs[0 if h == 0 else 1, t, pl.ds(w0, nblk), :] = blk.astype(BF16)
                        if pivot is None:
                            pivot = blk[0:1, :]
                        for k in range(nblk // 8):
                            d = blk[k * SUB:k * SUB + SUB] - pivot
                            s1 = s1 + d
                            s2 = s2 + d * d
            return pivot, s1, s2

        def stage(n, carry):
            b, s = n // 2, lax.rem(n, 2)
            latent_maps(b, s)
            for_dirs(lambda d: halo_copy(n, d, row_src), "recv")
            halo_rows(n)
            recv_stats(n, b, s)
            lax.fori_loop(0, 3, lambda h, c: (activate_row(n, h), c)[1], 0)
            ld_weight(n, b, s).wait()
            for_dirs(lambda d: halo_copy(n, d, row_src), "send")
            sums = (None, zero8, zero8)
            for h, ahead in zip(EDGE, ((HE - 3, HE - 2, HE - 1), (3, 4))):
                conv(n, (h,), range(NTAP))
                for k in ahead:
                    activate_row(n, k)
                sums = finish(b, s, (h,), sums)
            fill_columns(EDGE)
            conv(n, INNER, range(EARLY))
            for_dirs(lambda d: halo_copy(n + 1, d, row_src), "start", ROW_DIRS)
            for h in INNER:
                conv(n, (h,), range(EARLY, NTAP))
                sums = finish(b, s, (h,), sums)
            pivot, s1, s2 = sums

            @pl.when(n < 3)
            def _():
                send_stats(n + 1, pivot, s1, s2)

            fill_columns(INNER)
            for_dirs(lambda d: halo_copy(n + 1, d, row_src), "start", COL_DIRS)
            return carry

        lax.fori_loop(0, 4, stage, 0)

        lax.fori_loop(1, HE - 1, plain_row, 0)
        for_dirs(lambda d: halo_copy(4, d, row_src), "recv", ROW_DIRS)
        halo_rows(4)
        for h in (0, HE - 1):
            plain_row(h, 0)
        for_dirs(lambda d: halo_copy(4, d, row_src), "recv", COL_DIRS)
        lax.fori_loop(0, HE, plain_edges, 0)
        for_dirs(lambda d: halo_copy(4, d, row_src), "send")
        for n in range(4):
            for j in range(1, n_dev):
                stat_copy(n, j).wait_send()

    main()


def up_kernel(a_ref, wu, ub, out, o32, part, ob, o_sem):
    def out_copy(q, a, hp):
        return pltpu.make_async_copy(ob.at[hp, q, a], out.at[:, 2 * (q * 3 + hp) + a], o_sem.at[hp, q, a])

    def main(*accs):
        for acc in accs:
            pltpu.matmul_pop(acc)

        def row_taps(a):
            return [(1, 1)] if a is None else [(0, a), (2, a + 1)]

        groups = []
        for a in (None, 0, 1):
            for b in (None, 0, 1):
                groups.append((a, b, [(k, l, dh, kw) for k, dh in row_taps(a) for l, kw in row_taps(b)]))
        taps = [(g, tap) for g, grp in enumerate(groups) for tap in grp[2]]

        def push(i):
            k, l, _, _ = taps[i % len(taps)][1]
            for q in PAIR:
                pltpu.matmul_push_rhs(wu[k, l], staging_register=0, mxu_index=q, transpose=True)

        def blocks(q, slot):
            va = pltpu.matmul_pop(accs[q * 6 + slot * 2])
            vb = pltpu.matmul_pop(accs[q * 6 + slot * 2 + 1])
            return va, vb

        push(0)
        for hp in TRIO:
            for i, (g, (k, l, dh, kw)) in enumerate(taps):
                slot = g % 3
                for q in PAIR:
                    pltpu.matmul_acc_lhs(accs[q * 6 + slot * 2], a_ref[kw, q * 3 + hp + dh, pl.ds(32, NA), :], load_staged_rhs=0)
                if hp < 2 or i + 1 < len(taps):
                    push(i + 1)
                for q in PAIR:
                    pltpu.matmul_acc_lhs(accs[q * 6 + slot * 2 + 1], a_ref[kw, q * 3 + hp + dh, pl.ds(ABASE + 32, NB), :])
                if i + 1 < len(taps) and taps[i + 1][0] == g:
                    continue
                a, b, _ = groups[g]
                for q in PAIR:
                    va, vb = blocks(q, slot)
                    for v, sl in ((va, pl.ds(0, NA)), (vb, pl.ds(NA, NB))):
                        if a is None and b is None:
                            part[q, 0, sl, :] = v + ub[...]
                        elif a is None:
                            part[q, 1 + b, sl, :] = v + part[q, 0, sl, :]
                        elif b is None:
                            part[q, 3, sl, :] = v
                    if a is None or b is None:
                        continue
                    va = va + part[q, 1 + b, pl.ds(0, NA), :] + part[q, 3, pl.ds(0, NA), :]
                    vb = vb + part[q, 1 + b, pl.ds(NA, NB), :] + part[q, 3, pl.ds(NA, NB), :]
                    for half in PAIR:
                        ln = slice(half * LN, half * LN + LN)
                        for t in range(T):
                            o32[q, half, pl.ds(t * 2 * W + b, TR, stride=2), :] = va[t * TR:t * TR + TR, ln]
                            kb = (t % T2) * TR + (t // T2) * 8
                            o32[q, half, pl.ds(t * 48 + 32 + b, 8, stride=2), :] = vb[kb:kb + 8, ln]
                    if b == 1:
                        for t in range(T):
                            for half in PAIR:
                                ob[hp, q, a, t, :, lanes(half)] = o32[q, half, pl.ds(t * 2 * W, 2 * W), :].astype(BF16)
                        out_copy(q, a, hp).start()
        for hp in TRIO:
            for q in PAIR:
                for a in PAIR:
                    out_copy(q, a, hp).wait()

    pl.run_scoped(main, *acc_specs())


def solution(mesh):
    n_sh, n_sw = mesh.shape["sh"], mesh.shape["sw"]
    n_dev = n_sh * n_sw
    vmem = pl.BlockSpec(memory_space=pltpu.VMEM)
    hbm = pl.BlockSpec(memory_space=pltpu.HBM)
    dma = pltpu.SemaphoreType.DMA
    vec, mat = pltpu.VMEM((2, 2, C), F32), pltpu.VMEM((2, 2, LZ, C), BF16)

    def local_step(features, latent, gn_gain, gn_bias, zy_weight, zy_bias, zb_weight, zb_bias, conv_weight, conv_bias, up_weight, up_bias):
        feat = features[0].transpose(1, 2, 3, 0)
        lat = latent[0].transpose(1, 2, 0, 3)
        cw = conv_weight.transpose(0, 1, 4, 5, 6, 2, 3).reshape(2, 2, 27, C, C)
        uw = up_weight.transpose(2, 3, 0, 1)
        aup = pl.pallas_call(
            functools.partial(stage_kernel, n_sh, n_sw),
            out_shape=jax.ShapeDtypeStruct((3, HE, AR, C), BF16),
            in_specs=[hbm] * 10,
            out_specs=vmem,
            scratch_shapes=[
                pltpu.VMEM((4, 27, C, C), BF16),
                pltpu.VMEM((3, HE, AR, C), BF16),
                pltpu.VMEM((2, HE * FR, 128), F32),
                pltpu.VMEM((H, FR, C), F32),
                pltpu.VMEM((H, FR, C), F32),
                pltpu.VMEM((HE + 1, FR, C), F32),
                pltpu.VMEM((HE + 1, FR, C), F32),
                pltpu.VMEM((HE + 1, FR, 128), BF16),
                pltpu.VMEM((H * FR + 96, 128), F32),
                pltpu.VMEM((T, H, LZ, W), BF16),
                pltpu.VMEM((T, H, W, C), BF16),
                pltpu.VMEM((5, 2, T, W, C), BF16),
                pltpu.VMEM((5, 2, HE, 16, C), BF16),
                pltpu.VMEM((2, T, W, C), BF16),
                pltpu.VMEM((2, H, 16, C), BF16),
                pltpu.VMEM((2, H * 16, 128), BF16),
                pltpu.VMEM((HE, 2, T * SW_, LN), F32),
                pltpu.VMEM((LN, 2 * C), BF16),
                pltpu.VMEM((4, 1, LN), F32),
                pltpu.VMEM((4, n_dev, 1, LN), F32),
                pltpu.VMEM((3, 8, C), F32),
                vec, vec, mat, vec, mat, vec, vec,
                dma((9,)), dma((4,)), dma((5, 8)), dma((5, 8)), dma((8,)), dma((8,)), dma((4, n_dev)), dma((4, n_dev)),
            ],
            compiler_params=pltpu.CompilerParams(collective_id=0, has_side_effects=True, vmem_limit_bytes=42 << 20),
            name="stages",
        )(*[pltpu.with_memory_space_constraint(v, pltpu.HBM) for v in (feat, lat, gn_gain, gn_bias, zy_weight, zy_bias, zb_weight, zb_bias, cw, conv_bias)])
        out = pl.pallas_call(
            up_kernel,
            out_shape=jax.ShapeDtypeStruct((T, 2 * H, 2 * W, C), BF16),
            in_specs=[vmem] * 3,
            out_specs=hbm,
            scratch_shapes=[
                pltpu.VMEM((2, 2, T * 2 * W, LN), F32),
                pltpu.VMEM((2, 4, FR, C), F32),
                pltpu.VMEM((3, 2, 2, T, 2 * W, C), BF16),
                dma((3, 2, 2)),
            ],
            compiler_params=pltpu.CompilerParams(vmem_limit_bytes=24 << 20),
            name="upsample",
        )(aup, uw, up_bias.reshape(1, C))
        return out.transpose(3, 0, 1, 2)[None]

    data_spec = P("dp", None, None, "sh", "sw")
    return jax.shard_map(local_step, mesh=mesh, in_specs=(data_spec, data_spec) + (P(),) * 10, out_specs=data_spec, check_vma=False)
```

```python
import functools

import jax
import jax.numpy as jnp
from jax import lax
from jax.experimental import pallas as pl
from jax.experimental.pallas import tpu as pltpu
from jax.sharding import PartitionSpec as P

GN_EPSILON = 1e-6
MESH = pl.DeviceIdType.MESH
F32 = jnp.float32
CONTRACT_LAST = (((1,), (1,)), ((), ()))
BF16 = jnp.bfloat16
T, H, W, C, LZ = 12, 6, 24, 256, 16
HE = H + 2
FR = T * W
NA, NB = T * 16, T * 8
AR = (T + 2) * 16 + (T // 2 + 2) * 16
ABASE = (T + 2) * 16
SW_ = 40
T2 = T // 2
dirs = [(-1, 0), (1, 0), (0, -1), (0, 1), (-1, -1), (-1, 1), (1, -1), (1, 1)]
ROW_DIRS, COL_DIRS = (0, 1, 4, 5, 6, 7), (2, 3)
EDGE, INNER = (0, H - 1), range(1, H - 1)


LN = 128
PAIR, TRIO = range(2), range(3)
GAPS = (1, 2, 4)
TAPS = [kt * 9 + kh * 3 + kw for kh in TRIO for kt in TRIO for kw in TRIO]
EARLY = 6
TR, SUB = 16, 8


def lanes(half):
    return pl.ds(half * LN, LN)


def tile(i):
    return pl.ds(i * TR, TR)


def chan(ref, b, s):
    return ref[b, pl.ds(s, 1), :]


def acc_specs():
    specs = []
    for q in PAIR:
        for _ in TRIO:
            specs += [pltpu.ACC(q)((NA, C), F32), pltpu.ACC(q)((NB, C), F32)]
    return specs


def write_operand(a_ref, s_ref, h, body_kw=TRIO, tail_kw=TRIO):
    for half in PAIR:
        ln = lanes(half)
        for kw in body_kw:
            for t in range(T):
                body = s_ref[h, half, pl.ds(t * SW_ + 7 + kw, TR), :].astype(BF16)
                a_ref[kw, h, tile(t + 2), ln] = body
                if t == 0:
                    a_ref[kw, h, tile(0), ln] = body
                    a_ref[kw, h, tile(1), ln] = body
        for kw in tail_kw:
            tails = [s_ref[h, half, pl.ds(t * SW_ + 23 + kw, SUB), :] for t in range(T)]
            pairs = [(max(t, 0), t + T2) for t in range(-2, T2)]
            for i, (p, n) in enumerate(pairs):
                both = jnp.concatenate([tails[p], tails[n]], axis=0).astype(BF16)
                a_ref[kw, h, pl.ds(ABASE + i * TR, TR), ln] = both


def stage_kernel(n_sh, n_sw, feat, lat, gain_in, gbias_in, zyw_in, zyb_in, zbw_in, zbb_in, cw, cb_in,
                 aup,
                 wv, a_ref, rx, xres, cv, yv, bv, lt, ltf, lv, fb, re, ce, rs, cs, lts, sv, wz,
                 stat_out, stat_in, par, gain, gbias, zyw, zyb, zbw, zbb, cb,
                 ld_sem, w_sem, hs_sem, hr_sem, ls_sem, lr_sem, ss_sem, sr_sem):
    n_dev = n_sh * n_sw
    sh = lax.axis_index("sh")
    sw = lax.axis_index("sw")
    me = sh * n_sw + sw
    has = {"u": sh > 0, "d": sh < n_sh - 1, "l": sw > 0, "r": sw < n_sw - 1}

    ld_feat = pltpu.make_async_copy(feat, fb, ld_sem.at[0])
    ld_lat = pltpu.make_async_copy(lat, lv, ld_sem.at[1])
    ld_lat.start()
    ld_feat.start()
    params = ((gain_in, gain), (gbias_in, gbias), (zyw_in, zyw), (zyb_in, zyb), (zbw_in, zbw), (zbb_in, zbb), (cb_in, cb))
    ld_params = [pltpu.make_async_copy(src, dst, ld_sem.at[2 + i]) for i, (src, dst) in enumerate(params)]
    for ld in ld_params:
        ld.start()

    def ld_weight(n, b, s):
        return pltpu.make_async_copy(cw.at[b, s], wv.at[n], w_sem.at[n])

    for n in range(4):
        ld_weight(n, n // 2, n % 2).start()

    zero_rows = jnp.zeros((FR, 128), BF16)
    for i in (0, HE - 1, HE):
        lt[i] = zero_rows

    def peer_of(j):
        p = lax.rem(me + j, n_dev)
        return p, {"sh": p // n_sw, "sw": lax.rem(p, n_sw)}

    bar = pltpu.get_barrier_semaphore()
    for j in range(1, n_dev):
        pl.semaphore_signal(bar, inc=1, device_id=peer_of(j)[1], device_id_type=MESH)


    def exists(dy, dx):
        c = None
        for cond, use in ((has["u"], dy < 0), (has["d"], dy > 0), (has["l"], dx < 0), (has["r"], dx > 0)):
            if use:
                c = cond if c is None else jnp.logical_and(c, cond)
        return c

    def device(dy, dx):
        return {"sh": sh + dy, "sw": sw + dx}

    def halo_refs(e, dy, dx, src0):
        side = 1 if dx < 0 else 0
        row = HE - 1 if dy < 0 else 0
        if dx == 0:
            src = (src0[0] if dy < 0 else src0[1])
            return src, re.at[e, 1 if dy < 0 else 0]
        col = 0 if dx < 0 else 1
        if dy == 0:
            return cs.at[col], ce.at[e, side, pl.ds(1, H)]
        return cs.at[col, 0 if dy < 0 else H - 1], ce.at[e, side, row]

    def halo_copy(e, d, src0):
        dy, dx = dirs[d]
        src, dst = halo_refs(e, dy, dx, src0)
        return pltpu.make_async_remote_copy(src_ref=src, dst_ref=dst, send_sem=hs_sem.at[e, d],
                                            recv_sem=hr_sem.at[e, d], device_id=device(dy, dx), device_id_type=MESH)

    def lat_copy(d):
        dy, dx = dirs[d]
        if dx == 0:
            src, dst = (lt.at[1], lt.at[HE - 1]) if dy < 0 else (lt.at[H], lt.at[0])
        else:
            col = 0 if dx < 0 else 1
            base = 128 if dx < 0 else 0
            if dy == 0:
                src, dst = lts.at[col], lt.at[HE, pl.ds(base + 16, H * 16)]
            else:
                row = 0 if dy < 0 else H - 1
                there = (HE - 1 if dy < 0 else 0) * 16
                src, dst = lts.at[col, tile(row)], lt.at[HE, pl.ds(base + there, 16)]
        return pltpu.make_async_remote_copy(src_ref=src, dst_ref=dst, send_sem=ls_sem.at[d],
                                            recv_sem=lr_sem.at[d], device_id=device(dy, dx), device_id_type=MESH)

    def for_dirs(make, what, which=ROW_DIRS + COL_DIRS):
        for d in which:
            dy, dx = dirs[d]
            if what == "recv":
                @pl.when(exists(-dy, -dx))
                def _(d=d):
                    make(d).wait_recv()
            else:
                @pl.when(exists(dy, dx))
                def _(d=d):
                    if what == "start":
                        make(d).start()
                    else:
                        make(d).wait_send()

    def stat_copy(n, j):
        p, dev = peer_of(j)
        return pltpu.make_async_remote_copy(src_ref=stat_out.at[n], dst_ref=stat_in.at[n, me], send_sem=ss_sem.at[n, j],
                                            recv_sem=sr_sem.at[n, me], device_id=dev, device_id_type=MESH)

    lane = lax.broadcasted_iota(jnp.int32, (1, LN), 1) & 7

    def partner(v, gap):
        return jnp.where((lane & gap) == 0, pltpu.roll(v, LN - gap, 1), pltpu.roll(v, gap, 1))

    def stack(v):
        return jnp.concatenate([v[:, :LN], v[:, LN:]], axis=0)

    def send_stats(n, pivot, s1, s2):
        count = 1.0 / (T * H * W)
        s1 = jnp.sum(s1, axis=0, keepdims=True) * count
        s2 = jnp.sum(s2, axis=0, keepdims=True) * count
        mean, var = stack(pivot + s1), stack(jnp.maximum(s2 - s1 * s1, 0.0))
        for gap in GAPS:
            mp, vp = partner(mean, gap), partner(var, gap)
            half_gap = (mean - mp) * 0.5
            var = (var + vp) * 0.5 + half_gap * half_gap
            mean = (mean + mp) * 0.5
        quad = (mean[0:1], mean[1:2], var[0:1], var[1:2])
        row = sum(jnp.where(lane == i, v, 0.0) for i, v in enumerate(quad))
        stat_out[n] = row
        stat_in[n, me] = row
        for j in range(1, n_dev):
            stat_copy(n, j).start()

    def recv_stats(n, b, s):
        for j in range(1, n_dev):
            p, dev = peer_of(j)
            pltpu.make_async_remote_copy(src_ref=stat_out.at[n], dst_ref=stat_in.at[n, p], send_sem=ss_sem.at[n, j],
                                         recv_sem=sr_sem.at[n, p], device_id=dev, device_id_type=MESH).wait_recv()
        vals = [stat_in[n, i] for i in range(n_dev)]
        total = functools.reduce(jnp.add, vals) * (1.0 / n_dev)
        between = functools.reduce(jnp.add, [jnp.square(v - total) for v in vals]) * (1.0 / n_dev)

        def pick(v, i):
            return jnp.where(lane == i, v, 0.0)

        x = jnp.concatenate([pick(total, 0), pick(total, 1), pick(total, 2) + pick(between, 0), pick(total, 3) + pick(between, 1)], axis=0)
        for gap in GAPS:
            x = x + partner(x, gap)
        mean = jnp.concatenate([x[0:1], x[1:2]], axis=1)
        rstd = lax.rsqrt(jnp.concatenate([x[2:3], x[3:4]], axis=1) + GN_EPSILON)
        par[0] = jnp.broadcast_to(mean, (SUB, C))
        par[1] = jnp.broadcast_to(rstd * chan(gain, b, s), (SUB, C))
        par[2] = jnp.broadcast_to(chan(gbias, b, s), (SUB, C))

    def fill_columns(rows):
        for h in rows:
            for side, w in ((0, 0), (1, W - 1)):
                for half in PAIR:
                    v = rx[half, pl.ds((h + 1) * FR + w, TR, stride=W), :]
                    cs[side, h, :, lanes(half)] = v.astype(BF16)

    def main():
        wz[...] = jnp.zeros(wz.shape, BF16)
        ltf[...] = jnp.zeros(ltf.shape, F32)
        ld_lat.wait()

        def turn_row(h, c):
            for t in range(T):
                ltf[pl.ds(h * FR + t * W, W), pl.ds(0, LZ)] = lv[t, h].astype(F32).T
            lt[h + 1] = ltf[pl.ds(pl.multiple_of(h * FR, TR), FR), :].astype(BF16)
            return c

        lax.fori_loop(0, H, turn_row, 0)
        for h in range(H):
            for side, w in ((0, 0), (1, W - 1)):
                lts[side, tile(h), :] = ltf[pl.ds(h * FR + w, TR, stride=W), :].astype(BF16)

        ld_feat.wait()
        pivot0 = fb[0, 0, pl.ds(0, 8), :].astype(F32)[0:1, :]
        pivot8 = jnp.broadcast_to(pivot0, (SUB, C))

        def load_row(h, carry):
            s1, s2 = carry
            for t in range(T):
                x = fb[t, h].astype(F32)
                for half in PAIR:
                    rx[half, pl.ds((h + 1) * FR + t * W, W), :] = x[:, half * LN:half * LN + LN]
                xres[h, pl.ds(t * W, W), :] = x
                for i in TRIO:
                    d = x[i * SUB:i * SUB + SUB] - pivot8
                    s1 = s1 + d
                    s2 = s2 + d * d
            return s1, s2

        zero8 = jnp.zeros((SUB, C), F32)
        s1, s2 = lax.fori_loop(0, H, load_row, (zero8, zero8))
        for t in range(T):
            rs[0, t] = fb[t, 0]
            rs[1, t] = fb[t, H - 1]
        fill_columns(range(H))
        row_src = (rs.at[0], rs.at[1])
        pl.semaphore_wait(bar, n_dev - 1)
        send_stats(0, pivot0, s1, s2)
        for_dirs(lat_copy, "start")
        for_dirs(lambda d: halo_copy(0, d, row_src), "start")
        for ld in ld_params:
            ld.wait()
        for_dirs(lat_copy, "recv")
        for_dirs(lat_copy, "send")

        half_or_zero = {k: jnp.where(v, 0.5, 0.0).astype(F32) for k, v in has.items()}

        def latent_maps(b, s):
            wz[pl.ds(0, LZ), pl.ds(0, C)] = zyw[b, s]
            wz[pl.ds(0, LZ), pl.ds(C, C)] = zbw[b, s]
            biases = (chan(zyb, b, s), chan(zbb, b, s))
            for i in range(HE + 1):
                v = jnp.dot(lt[i], wz[...], preferred_element_type=F32)
                for q, out in ((0, yv), (1, bv)):
                    m = v[:, q * C:q * C + C] + biases[q]
                    if i < HE:
                        f = half_or_zero["u"] if i == 0 else half_or_zero["d"] if i == HE - 1 else 0.5
                        out[i] = m * f
                    else:
                        for seg in range(2 * HE):
                            f = half_or_zero["l" if seg < HE else "r"]
                            if seg % HE == 0:
                                f = f * half_or_zero["u"] * 2.0
                            if seg % HE == HE - 1:
                                f = f * half_or_zero["d"] * 2.0
                            out[i, tile(seg), :] = m[seg * TR:seg * TR + TR] * f

        def activate(x, y, b):
            n = x.shape[0] // 8
            x, y, b = (v.reshape(n, 8, C) for v in (x, y, b))
            hv = ((x - par[0][None]) * par[1][None] + par[2][None]) * y + b
            return (hv * jnp.tanh(hv) + hv).reshape(n * 8, C)

        def halo_rows(e):
            for i, cond in ((0, has["u"]), (1, has["d"])):
                row = 0 if i == 0 else HE - 1
                for t in range(T):
                    v = jnp.where(cond, re[e, i, t].astype(F32), 0.0)
                    for half in PAIR:
                        rx[half, pl.ds(row * FR + t * W, W), :] = v[:, half * LN:half * LN + LN]

        def col_vals(e, side, h):
            cond = has["l"] if side == 0 else has["r"]
            cond = jnp.logical_and(cond, jnp.logical_or(jnp.int32(h) > 0, has["u"]))
            cond = jnp.logical_and(cond, jnp.logical_or(jnp.int32(h) < HE - 1, has["d"]))
            return jnp.where(cond, ce[e, side, h].astype(F32), 0.0)

        def put_column(h, side, v):
            for half in PAIR:
                sv[h, half, pl.ds(7 + side * 25, T, stride=SW_), :] = v[0:T, half * LN:half * LN + LN]

        def own_rows(h, t, half):
            return rx[half, pl.ds(pl.multiple_of(h * FR, SUB) + t * W, W), :]

        def activate_row(n, h):
            for side in PAIR:
                at = pl.ds(pl.multiple_of(side * LN + h * TR, TR), TR)
                put_column(h, side, activate(col_vals(n, side, h), yv[HE, at, :], bv[HE, at, :]))
            for t in range(T):
                x = jnp.concatenate([own_rows(h, t, half) for half in PAIR], axis=1)
                v = activate(x, yv[h, pl.ds(t * W, W), :], bv[h, pl.ds(t * W, W), :])
                for half in PAIR:
                    sv[h, half, pl.ds(t * SW_ + 8, W), :] = v[:, half * LN:half * LN + LN]
            write_operand(a_ref, sv, h)

        def plain_row(h, c):
            for t in range(T):
                for half in PAIR:
                    sv[h, half, pl.ds(t * SW_ + 8, W), :] = own_rows(h, t, half)
            write_operand(aup, sv, h)
            return c

        def plain_edges(h, c):
            for side in PAIR:
                put_column(h, side, col_vals(4, side, h))
            write_operand(aup, sv, h, (0,), (2,))
            return c

        def conv(n, rows, taps):
            def lhs(h, part, tap):
                kt, kh, kw = tap // 9, tap // 3 % 3, tap % 3
                return a_ref[kw, h + kh, pl.ds(kt * 16 + (ABASE if part else 0), NB if part else NA), :]

            for h in rows:
                rhs = jnp.concatenate([wv[n, i] for i in taps], axis=1)
                cols = [jnp.concatenate([lhs(h, part, i) for part in PAIR], axis=0) for i in taps]
                v = lax.dot_general(jnp.concatenate(cols, axis=1), rhs, CONTRACT_LAST, preferred_element_type=F32)
                if taps[0] == 0:
                    cv[h] = v
                else:
                    cv[h] += v

        def finish(b, s, rows, sums):
            bias = chan(cb, b, s)
            second = s == 1
            pivot, s1, s2 = sums
            for h in rows:
                for part in PAIR:
                    v = (cv[h, pl.ds(NA if part else 0, NB if part else NA), :] + bias).astype(BF16).astype(F32)
                    nblk = 16 if part == 0 else 8
                    for i in range(T):
                        if part == 0:
                            t, w0 = i, 0
                        else:
                            t, w0 = (i // 2) + (i % 2) * T2, 16
                        blk = v[i * nblk:(i + 1) * nblk]
                        r0 = t * W + w0
                        res = xres[h, pl.ds(r0, nblk), :]
                        blk = (blk + jnp.where(second, res, 0.0)).astype(BF16).astype(F32)
                        xres[h, pl.ds(r0, nblk), :] = jnp.where(second, blk, res)
                        for half in PAIR:
                            rx[half, pl.ds((h + 1) * FR + r0, nblk), :] = blk[:, half * LN:half * LN + LN]
                        if h in (0, H - 1):
                            rs[0 if h == 0 else 1, t, pl.ds(w0, nblk), :] = blk.astype(BF16)
                        if pivot is None:
                            pivot = blk[0:1, :]
                        for k in range(nblk // 8):
                            d = blk[k * SUB:k * SUB + SUB] - pivot
                            s1 = s1 + d
                            s2 = s2 + d * d
            return pivot, s1, s2

        def stage(n, carry):
            b, s = n // 2, lax.rem(n, 2)
            latent_maps(b, s)
            for_dirs(lambda d: halo_copy(n, d, row_src), "recv")
            halo_rows(n)
            recv_stats(n, b, s)
            ld_weight(n, b, s).wait()
            for_dirs(lambda d: halo_copy(n, d, row_src), "send")
            for h in TRIO:
                activate_row(n, h)
            sums = (None, zero8, zero8)
            for h, ahead in zip(EDGE, ((HE - 3, HE - 2, HE - 1), (3, 4))):
                conv(n, (h,), TAPS)
                for k in ahead:
                    activate_row(n, k)
                sums = finish(b, s, (h,), sums)
            fill_columns(EDGE)
            conv(n, INNER, TAPS[:EARLY])
            for_dirs(lambda d: halo_copy(n + 1, d, row_src), "start", ROW_DIRS)
            for h in INNER:
                conv(n, (h,), TAPS[EARLY:])
                sums = finish(b, s, (h,), sums)
            pivot, s1, s2 = sums

            @pl.when(n < 3)
            def _():
                send_stats(n + 1, pivot, s1, s2)

            fill_columns(INNER)
            for_dirs(lambda d: halo_copy(n + 1, d, row_src), "start", COL_DIRS)
            return carry

        lax.fori_loop(0, 4, stage, 0)

        lax.fori_loop(1, HE - 1, plain_row, 0)
        for_dirs(lambda d: halo_copy(4, d, row_src), "recv", ROW_DIRS)
        halo_rows(4)
        for h in (0, HE - 1):
            plain_row(h, 0)
        for_dirs(lambda d: halo_copy(4, d, row_src), "recv", COL_DIRS)
        lax.fori_loop(0, HE, plain_edges, 0)
        for_dirs(lambda d: halo_copy(4, d, row_src), "send")
        for n in range(4):
            for j in range(1, n_dev):
                stat_copy(n, j).wait_send()

    main()


def up_kernel(a_ref, wu, ub, out, o32, part, ob, o_sem):
    def out_copy(q, a, hp):
        return pltpu.make_async_copy(ob.at[hp, q, a], out.at[:, 2 * (q * 3 + hp) + a], o_sem.at[hp, q, a])

    def main(*accs):
        for acc in accs:
            pltpu.matmul_pop(acc)

        def row_taps(a):
            return [(1, 1)] if a is None else [(0, a), (2, a + 1)]

        groups = []
        for a in (None, 0, 1):
            for b in (None, 0, 1):
                groups.append((a, b, [(k, l, dh, kw) for k, dh in row_taps(a) for l, kw in row_taps(b)]))
        taps = [(g, tap) for g, grp in enumerate(groups) for tap in grp[2]]

        def push(i):
            k, l, _, _ = taps[i % len(taps)][1]
            for q in PAIR:
                pltpu.matmul_push_rhs(wu[k, l], staging_register=0, mxu_index=q, transpose=True)

        def blocks(q, slot):
            va = pltpu.matmul_pop(accs[q * 6 + slot * 2])
            vb = pltpu.matmul_pop(accs[q * 6 + slot * 2 + 1])
            return va, vb

        push(0)
        for hp in TRIO:
            for i, (g, (k, l, dh, kw)) in enumerate(taps):
                slot = g % 3
                for q in PAIR:
                    pltpu.matmul_acc_lhs(accs[q * 6 + slot * 2], a_ref[kw, q * 3 + hp + dh, pl.ds(32, NA), :], load_staged_rhs=0)
                if hp < 2 or i + 1 < len(taps):
                    push(i + 1)
                for q in PAIR:
                    pltpu.matmul_acc_lhs(accs[q * 6 + slot * 2 + 1], a_ref[kw, q * 3 + hp + dh, pl.ds(ABASE + 32, NB), :])
                if i + 1 < len(taps) and taps[i + 1][0] == g:
                    continue
                a, b, _ = groups[g]
                for q in PAIR:
                    va, vb = blocks(q, slot)
                    for v, sl in ((va, pl.ds(0, NA)), (vb, pl.ds(NA, NB))):
                        if a is None and b is None:
                            part[q, 0, sl, :] = v + ub[...]
                        elif a is None:
                            part[q, 1 + b, sl, :] = v + part[q, 0, sl, :]
                        elif b is None:
                            part[q, 3, sl, :] = v
                    if a is None or b is None:
                        continue
                    va = va + part[q, 1 + b, pl.ds(0, NA), :] + part[q, 3, pl.ds(0, NA), :]
                    vb = vb + part[q, 1 + b, pl.ds(NA, NB), :] + part[q, 3, pl.ds(NA, NB), :]
                    for half in PAIR:
                        ln = slice(half * LN, half * LN + LN)
                        for t in range(T):
                            o32[q, half, pl.ds(t * 2 * W + b, TR, stride=2), :] = va[t * TR:t * TR + TR, ln]
                            kb = (t % T2) * TR + (t // T2) * 8
                            o32[q, half, pl.ds(t * 48 + 32 + b, 8, stride=2), :] = vb[kb:kb + 8, ln]
                    if b == 1:
                        for t in range(T):
                            for half in PAIR:
                                ob[hp, q, a, t, :, lanes(half)] = o32[q, half, pl.ds(t * 2 * W, 2 * W), :].astype(BF16)
                        out_copy(q, a, hp).start()
        for hp in TRIO:
            for q in PAIR:
                for a in PAIR:
                    out_copy(q, a, hp).wait()

    pl.run_scoped(main, *acc_specs())


def solution(mesh):
    n_sh, n_sw = mesh.shape["sh"], mesh.shape["sw"]
    n_dev = n_sh * n_sw
    vmem = pl.BlockSpec(memory_space=pltpu.VMEM)
    hbm = pl.BlockSpec(memory_space=pltpu.HBM)
    dma = pltpu.SemaphoreType.DMA
    vec, mat = pltpu.VMEM((2, 2, C), F32), pltpu.VMEM((2, 2, LZ, C), BF16)

    def local_step(features, latent, gn_gain, gn_bias, zy_weight, zy_bias, zb_weight, zb_bias, conv_weight, conv_bias, up_weight, up_bias):
        feat = features[0].transpose(1, 2, 3, 0)
        lat = latent[0].transpose(1, 2, 0, 3)
        cw = conv_weight.transpose(0, 1, 4, 5, 6, 2, 3).reshape(2, 2, 27, C, C)
        uw = up_weight.transpose(2, 3, 0, 1)
        aup = pl.pallas_call(
            functools.partial(stage_kernel, n_sh, n_sw),
            out_shape=jax.ShapeDtypeStruct((3, HE, AR, C), BF16),
            in_specs=[hbm] * 10,
            out_specs=vmem,
            scratch_shapes=[
                pltpu.VMEM((4, 27, C, C), BF16),
                pltpu.VMEM((3, HE, AR, C), BF16),
                pltpu.VMEM((2, HE * FR, 128), F32),
                pltpu.VMEM((H, FR, C), F32),
                pltpu.VMEM((H, FR, C), F32),
                pltpu.VMEM((HE + 1, FR, C), F32),
                pltpu.VMEM((HE + 1, FR, C), F32),
                pltpu.VMEM((HE + 1, FR, 128), BF16),
                pltpu.VMEM((H * FR + 96, 128), F32),
                pltpu.VMEM((T, H, LZ, W), BF16),
                pltpu.VMEM((T, H, W, C), BF16),
                pltpu.VMEM((5, 2, T, W, C), BF16),
                pltpu.VMEM((5, 2, HE, 16, C), BF16),
                pltpu.VMEM((2, T, W, C), BF16),
                pltpu.VMEM((2, H, 16, C), BF16),
                pltpu.VMEM((2, H * 16, 128), BF16),
                pltpu.VMEM((HE, 2, T * SW_, LN), F32),
                pltpu.VMEM((LN, 2 * C), BF16),
                pltpu.VMEM((4, 1, LN), F32),
                pltpu.VMEM((4, n_dev, 1, LN), F32),
                pltpu.VMEM((3, 8, C), F32),
                vec, vec, mat, vec, mat, vec, vec,
                dma((9,)), dma((4,)), dma((5, 8)), dma((5, 8)), dma((8,)), dma((8,)), dma((4, n_dev)), dma((4, n_dev)),
            ],
            compiler_params=pltpu.CompilerParams(collective_id=0, has_side_effects=True, vmem_limit_bytes=42 << 20),
            name="stages",
        )(*[pltpu.with_memory_space_constraint(v, pltpu.HBM) for v in (feat, lat, gn_gain, gn_bias, zy_weight, zy_bias, zb_weight, zb_bias, cw, conv_bias)])
        out = pl.pallas_call(
            up_kernel,
            out_shape=jax.ShapeDtypeStruct((T, 2 * H, 2 * W, C), BF16),
            in_specs=[vmem] * 3,
            out_specs=hbm,
            scratch_shapes=[
                pltpu.VMEM((2, 2, T * 2 * W, LN), F32),
                pltpu.VMEM((2, 4, FR, C), F32),
                pltpu.VMEM((3, 2, 2, T, 2 * W, C), BF16),
                dma((3, 2, 2)),
            ],
            compiler_params=pltpu.CompilerParams(vmem_limit_bytes=24 << 20),
            name="upsample",
        )(aup, uw, up_bias.reshape(1, C))
        return out.transpose(3, 0, 1, 2)[None]

    data_spec = P("dp", None, None, "sh", "sw")
    return jax.shard_map(local_step, mesh=mesh, in_specs=(data_spec, data_spec) + (P(),) * 10, out_specs=data_spec, check_vma=False)
```

```python
import functools

import jax
import jax.numpy as jnp
from jax import lax
from jax.experimental import pallas as pl
from jax.experimental.pallas import tpu as pltpu
from jax.sharding import PartitionSpec as P

GN_EPSILON = 1e-6
MESH = pl.DeviceIdType.MESH
F32 = jnp.float32
CONTRACT_LAST = (((1,), (1,)), ((), ()))
BF16 = jnp.bfloat16
T, H, W, C, LZ = 12, 6, 24, 256, 16
HE = H + 2
FR = T * W
NA, NB = T * 16, T * 8
AR = (T + 2) * 16 + (T // 2 + 2) * 16
ABASE = (T + 2) * 16
SW_ = 40
T2 = T // 2
dirs = [(-1, 0), (1, 0), (0, -1), (0, 1), (-1, -1), (-1, 1), (1, -1), (1, 1)]
ROW_DIRS, COL_DIRS = (0, 1, 4, 5, 6, 7), (2, 3)
EDGE, INNER = (0, H - 1), range(1, H - 1)


LN = 128
PAIR, TRIO = range(2), range(3)
GAPS = (1, 2, 4)
TAPS = [kt * 9 + kh * 3 + kw for kh in TRIO for kt in TRIO for kw in TRIO]
EARLY = 9
TR, SUB = 16, 8


def lanes(half):
    return pl.ds(half * LN, LN)


def tile(i):
    return pl.ds(i * TR, TR)


def chan(ref, b, s):
    return ref[b, pl.ds(s, 1), :]


def acc_specs():
    specs = []
    for q in PAIR:
        for _ in TRIO:
            specs += [pltpu.ACC(q)((NA, C), F32), pltpu.ACC(q)((NB, C), F32)]
    return specs


def write_operand(a_ref, s_ref, h, body_kw=TRIO, tail_kw=TRIO):
    for half in PAIR:
        ln = lanes(half)
        for kw in body_kw:
            for t in range(T):
                body = s_ref[h, half, pl.ds(t * SW_ + 7 + kw, TR), :].astype(BF16)
                a_ref[kw, h, tile(t + 2), ln] = body
                if t == 0:
                    a_ref[kw, h, tile(0), ln] = body
                    a_ref[kw, h, tile(1), ln] = body
        for kw in tail_kw:
            tails = [s_ref[h, half, pl.ds(t * SW_ + 23 + kw, SUB), :] for t in range(T)]
            pairs = [(max(t, 0), t + T2) for t in range(-2, T2)]
            for i, (p, n) in enumerate(pairs):
                both = jnp.concatenate([tails[p], tails[n]], axis=0).astype(BF16)
                a_ref[kw, h, pl.ds(ABASE + i * TR, TR), ln] = both


def stage_kernel(n_sh, n_sw, feat, lat, gain_in, gbias_in, zyw_in, zyb_in, zbw_in, zbb_in, cw, cb_in,
                 aup,
                 wv, a_ref, rx, xres, cv, yv, bv, lt, ltf, lv, fb, re, ce, rs, cs, lts, sv, wz,
                 stat_out, stat_in, par, gain, gbias, zyw, zyb, zbw, zbb, cb,
                 ld_sem, w_sem, hs_sem, hr_sem, ls_sem, lr_sem, ss_sem, sr_sem):
    n_dev = n_sh * n_sw
    sh = lax.axis_index("sh")
    sw = lax.axis_index("sw")
    me = sh * n_sw + sw
    has = {"u": sh > 0, "d": sh < n_sh - 1, "l": sw > 0, "r": sw < n_sw - 1}

    ld_feat = pltpu.make_async_copy(feat, fb, ld_sem.at[0])
    ld_lat = pltpu.make_async_copy(lat, lv, ld_sem.at[1])
    ld_lat.start()
    ld_feat.start()
    params = ((gain_in, gain), (gbias_in, gbias), (zyw_in, zyw), (zyb_in, zyb), (zbw_in, zbw), (zbb_in, zbb), (cb_in, cb))
    ld_params = [pltpu.make_async_copy(src, dst, ld_sem.at[2 + i]) for i, (src, dst) in enumerate(params)]
    for ld in ld_params:
        ld.start()

    def ld_weight(n, b, s):
        return pltpu.make_async_copy(cw.at[b, s], wv.at[n], w_sem.at[n])

    for n in range(4):
        ld_weight(n, n // 2, n % 2).start()

    zero_rows = jnp.zeros((FR, 128), BF16)
    for i in (0, HE - 1, HE):
        lt[i] = zero_rows

    def peer_of(j):
        p = lax.rem(me + j, n_dev)
        return p, {"sh": p // n_sw, "sw": lax.rem(p, n_sw)}

    bar = pltpu.get_barrier_semaphore()
    for j in range(1, n_dev):
        pl.semaphore_signal(bar, inc=1, device_id=peer_of(j)[1], device_id_type=MESH)


    def exists(dy, dx):
        c = None
        for cond, use in ((has["u"], dy < 0), (has["d"], dy > 0), (has["l"], dx < 0), (has["r"], dx > 0)):
            if use:
                c = cond if c is None else jnp.logical_and(c, cond)
        return c

    def device(dy, dx):
        return {"sh": sh + dy, "sw": sw + dx}

    def halo_refs(e, dy, dx, src0):
        side = 1 if dx < 0 else 0
        row = HE - 1 if dy < 0 else 0
        if dx == 0:
            src = (src0[0] if dy < 0 else src0[1])
            return src, re.at[e, 1 if dy < 0 else 0]
        col = 0 if dx < 0 else 1
        if dy == 0:
            return cs.at[col], ce.at[e, side, pl.ds(1, H)]
        return cs.at[col, 0 if dy < 0 else H - 1], ce.at[e, side, row]

    def halo_copy(e, d, src0):
        dy, dx = dirs[d]
        src, dst = halo_refs(e, dy, dx, src0)
        return pltpu.make_async_remote_copy(src_ref=src, dst_ref=dst, send_sem=hs_sem.at[e, d],
                                            recv_sem=hr_sem.at[e, d], device_id=device(dy, dx), device_id_type=MESH)

    def lat_copy(d):
        dy, dx = dirs[d]
        if dx == 0:
            src, dst = (lt.at[1], lt.at[HE - 1]) if dy < 0 else (lt.at[H], lt.at[0])
        else:
            col = 0 if dx < 0 else 1
            base = 128 if dx < 0 else 0
            if dy == 0:
                src, dst = lts.at[col], lt.at[HE, pl.ds(base + 16, H * 16)]
            else:
                row = 0 if dy < 0 else H - 1
                there = (HE - 1 if dy < 0 else 0) * 16
                src, dst = lts.at[col, tile(row)], lt.at[HE, pl.ds(base + there, 16)]
        return pltpu.make_async_remote_copy(src_ref=src, dst_ref=dst, send_sem=ls_sem.at[d],
                                            recv_sem=lr_sem.at[d], device_id=device(dy, dx), device_id_type=MESH)

    def for_dirs(make, what, which=ROW_DIRS + COL_DIRS):
        for d in which:
            dy, dx = dirs[d]
            if what == "recv":
                @pl.when(exists(-dy, -dx))
                def _(d=d):
                    make(d).wait_recv()
            else:
                @pl.when(exists(dy, dx))
                def _(d=d):
                    if what == "start":
                        make(d).start()
                    else:
                        make(d).wait_send()

    def stat_copy(n, j):
        p, dev = peer_of(j)
        return pltpu.make_async_remote_copy(src_ref=stat_out.at[n], dst_ref=stat_in.at[n, me], send_sem=ss_sem.at[n, j],
                                            recv_sem=sr_sem.at[n, me], device_id=dev, device_id_type=MESH)

    lane = lax.broadcasted_iota(jnp.int32, (1, LN), 1) & 7

    def partner(v, gap):
        return jnp.where((lane & gap) == 0, pltpu.roll(v, LN - gap, 1), pltpu.roll(v, gap, 1))

    def stack(v):
        return jnp.concatenate([v[:, :LN], v[:, LN:]], axis=0)

    def send_stats(n, pivot, s1, s2):
        count = 1.0 / (T * H * W)
        s1 = jnp.sum(s1, axis=0, keepdims=True) * count
        s2 = jnp.sum(s2, axis=0, keepdims=True) * count
        mean, var = stack(pivot + s1), stack(jnp.maximum(s2 - s1 * s1, 0.0))
        for gap in GAPS:
            mp, vp = partner(mean, gap), partner(var, gap)
            half_gap = (mean - mp) * 0.5
            var = (var + vp) * 0.5 + half_gap * half_gap
            mean = (mean + mp) * 0.5
        quad = (mean[0:1], mean[1:2], var[0:1], var[1:2])
        row = sum(jnp.where(lane == i, v, 0.0) for i, v in enumerate(quad))
        stat_out[n] = row
        stat_in[n, me] = row
        for j in range(1, n_dev):
            stat_copy(n, j).start()

    def recv_stats(n, b, s):
        for j in range(1, n_dev):
            p, dev = peer_of(j)
            pltpu.make_async_remote_copy(src_ref=stat_out.at[n], dst_ref=stat_in.at[n, p], send_sem=ss_sem.at[n, j],
                                         recv_sem=sr_sem.at[n, p], device_id=dev, device_id_type=MESH).wait_recv()
        vals = [stat_in[n, i] for i in range(n_dev)]
        total = functools.reduce(jnp.add, vals) * (1.0 / n_dev)
        between = functools.reduce(jnp.add, [jnp.square(v - total) for v in vals]) * (1.0 / n_dev)

        def pick(v, i):
            return jnp.where(lane == i, v, 0.0)

        x = jnp.concatenate([pick(total, 0), pick(total, 1), pick(total, 2) + pick(between, 0), pick(total, 3) + pick(between, 1)], axis=0)
        for gap in GAPS:
            x = x + partner(x, gap)
        mean = jnp.concatenate([x[0:1], x[1:2]], axis=1)
        rstd = lax.rsqrt(jnp.concatenate([x[2:3], x[3:4]], axis=1) + GN_EPSILON)
        par[0] = jnp.broadcast_to(mean, (SUB, C))
        par[1] = jnp.broadcast_to(rstd * chan(gain, b, s), (SUB, C))
        par[2] = jnp.broadcast_to(chan(gbias, b, s), (SUB, C))

    def fill_columns(rows):
        for h in rows:
            for side, w in ((0, 0), (1, W - 1)):
                for half in PAIR:
                    v = rx[half, pl.ds((h + 1) * FR + w, TR, stride=W), :]
                    cs[side, h, :, lanes(half)] = v.astype(BF16)

    def main():
        wz[...] = jnp.zeros(wz.shape, BF16)
        ltf[...] = jnp.zeros(ltf.shape, F32)
        ld_lat.wait()

        def turn_row(h, c):
            for t in range(T):
                ltf[pl.ds(h * FR + t * W, W), pl.ds(0, LZ)] = lv[t, h].astype(F32).T
            lt[h + 1] = ltf[pl.ds(pl.multiple_of(h * FR, TR), FR), :].astype(BF16)
            return c

        lax.fori_loop(0, H, turn_row, 0)
        for h in range(H):
            for side, w in ((0, 0), (1, W - 1)):
                lts[side, tile(h), :] = ltf[pl.ds(h * FR + w, TR, stride=W), :].astype(BF16)

        ld_feat.wait()
        pivot0 = fb[0, 0, pl.ds(0, 8), :].astype(F32)[0:1, :]
        pivot8 = jnp.broadcast_to(pivot0, (SUB, C))

        def load_row(h, carry):
            s1, s2 = carry
            for t in range(T):
                x = fb[t, h].astype(F32)
                for half in PAIR:
                    rx[half, pl.ds((h + 1) * FR + t * W, W), :] = x[:, half * LN:half * LN + LN]
                xres[h, pl.ds(t * W, W), :] = x
                for i in TRIO:
                    d = x[i * SUB:i * SUB + SUB] - pivot8
                    s1 = s1 + d
                    s2 = s2 + d * d
            return s1, s2

        zero8 = jnp.zeros((SUB, C), F32)
        s1, s2 = lax.fori_loop(0, H, load_row, (zero8, zero8))
        for t in range(T):
            rs[0, t] = fb[t, 0]
            rs[1, t] = fb[t, H - 1]
        fill_columns(range(H))
        row_src = (rs.at[0], rs.at[1])
        pl.semaphore_wait(bar, n_dev - 1)
        send_stats(0, pivot0, s1, s2)
        for_dirs(lat_copy, "start")
        for_dirs(lambda d: halo_copy(0, d, row_src), "start")
        for ld in ld_params:
            ld.wait()
        for_dirs(lat_copy, "recv")
        for_dirs(lat_copy, "send")

        half_or_zero = {k: jnp.where(v, 0.5, 0.0).astype(F32) for k, v in has.items()}

        def latent_maps(b, s):
            wz[pl.ds(0, LZ), pl.ds(0, C)] = zyw[b, s]
            wz[pl.ds(0, LZ), pl.ds(C, C)] = zbw[b, s]
            biases = (chan(zyb, b, s), chan(zbb, b, s))
            for i in range(HE + 1):
                v = jnp.dot(lt[i], wz[...], preferred_element_type=F32)
                for q, out in ((0, yv), (1, bv)):
                    m = v[:, q * C:q * C + C] + biases[q]
                    if i < HE:
                        f = half_or_zero["u"] if i == 0 else half_or_zero["d"] if i == HE - 1 else 0.5
                        out[i] = m * f
                    else:
                        for seg in range(2 * HE):
                            f = half_or_zero["l" if seg < HE else "r"]
                            if seg % HE == 0:
                                f = f * half_or_zero["u"] * 2.0
                            if seg % HE == HE - 1:
                                f = f * half_or_zero["d"] * 2.0
                            out[i, tile(seg), :] = m[seg * TR:seg * TR + TR] * f

        def activate(x, y, b):
            n = x.shape[0] // 8
            x, y, b = (v.reshape(n, 8, C) for v in (x, y, b))
            hv = ((x - par[0][None]) * par[1][None] + par[2][None]) * y + b
            return (hv * jnp.tanh(hv) + hv).reshape(n * 8, C)

        def halo_rows(e):
            for i, cond in ((0, has["u"]), (1, has["d"])):
                row = 0 if i == 0 else HE - 1
                for t in range(T):
                    v = jnp.where(cond, re[e, i, t].astype(F32), 0.0)
                    for half in PAIR:
                        rx[half, pl.ds(row * FR + t * W, W), :] = v[:, half * LN:half * LN + LN]

        def col_vals(e, side, h):
            cond = has["l"] if side == 0 else has["r"]
            cond = jnp.logical_and(cond, jnp.logical_or(jnp.int32(h) > 0, has["u"]))
            cond = jnp.logical_and(cond, jnp.logical_or(jnp.int32(h) < HE - 1, has["d"]))
            return jnp.where(cond, ce[e, side, h].astype(F32), 0.0)

        def put_column(h, side, v):
            for half in PAIR:
                sv[h, half, pl.ds(7 + side * 25, T, stride=SW_), :] = v[0:T, half * LN:half * LN + LN]

        def own_rows(h, t, half):
            return rx[half, pl.ds(pl.multiple_of(h * FR, SUB) + t * W, W), :]

        def activate_row(n, h):
            for side in PAIR:
                at = pl.ds(pl.multiple_of(side * LN + h * TR, TR), TR)
                put_column(h, side, activate(col_vals(n, side, h), yv[HE, at, :], bv[HE, at, :]))
            for t in range(T):
                x = jnp.concatenate([own_rows(h, t, half) for half in PAIR], axis=1)
                v = activate(x, yv[h, pl.ds(t * W, W), :], bv[h, pl.ds(t * W, W), :])
                for half in PAIR:
                    sv[h, half, pl.ds(t * SW_ + 8, W), :] = v[:, half * LN:half * LN + LN]
            write_operand(a_ref, sv, h)

        def plain_row(h, c):
            for t in range(T):
                for half in PAIR:
                    sv[h, half, pl.ds(t * SW_ + 8, W), :] = own_rows(h, t, half)
            write_operand(aup, sv, h)
            return c

        def plain_edges(h, c):
            for side in PAIR:
                put_column(h, side, col_vals(4, side, h))
            write_operand(aup, sv, h, (0,), (2,))
            return c

        def conv(n, rows, taps):
            def lhs(h, part, tap):
                kt, kh, kw = tap // 9, tap // 3 % 3, tap % 3
                return a_ref[kw, h + kh, pl.ds(kt * 16 + (ABASE if part else 0), NB if part else NA), :]

            for h in rows:
                rhs = jnp.concatenate([wv[n, i] for i in taps], axis=1)
                cols = [jnp.concatenate([lhs(h, part, i) for part in PAIR], axis=0) for i in taps]
                v = lax.dot_general(jnp.concatenate(cols, axis=1), rhs, CONTRACT_LAST, preferred_element_type=F32)
                if taps[0] == 0:
                    cv[h] = v
                else:
                    cv[h] += v

        def finish(b, s, rows, sums):
            bias = chan(cb, b, s)
            second = s == 1
            pivot, s1, s2 = sums
            for h in rows:
                for part in PAIR:
                    v = (cv[h, pl.ds(NA if part else 0, NB if part else NA), :] + bias).astype(BF16).astype(F32)
                    nblk = 16 if part == 0 else 8
                    for i in range(T):
                        if part == 0:
                            t, w0 = i, 0
                        else:
                            t, w0 = (i // 2) + (i % 2) * T2, 16
                        blk = v[i * nblk:(i + 1) * nblk]
                        r0 = t * W + w0
                        res = xres[h, pl.ds(r0, nblk), :]
                        blk = (blk + jnp.where(second, res, 0.0)).astype(BF16).astype(F32)
                        xres[h, pl.ds(r0, nblk), :] = jnp.where(second, blk, res)
                        for half in PAIR:
                            rx[half, pl.ds((h + 1) * FR + r0, nblk), :] = blk[:, half * LN:half * LN + LN]
                        if h in (0, H - 1):
                            rs[0 if h == 0 else 1, t, pl.ds(w0, nblk), :] = blk.astype(BF16)
                        if pivot is None:
                            pivot = blk[0:1, :]
                        for k in range(nblk // 8):
                            d = blk[k * SUB:k * SUB + SUB] - pivot
                            s1 = s1 + d
                            s2 = s2 + d * d
            return pivot, s1, s2

        def stage(n, carry):
            b, s = n // 2, lax.rem(n, 2)
            latent_maps(b, s)
            for_dirs(lambda d: halo_copy(n, d, row_src), "recv")
            halo_rows(n)
            recv_stats(n, b, s)
            ld_weight(n, b, s).wait()
            for_dirs(lambda d: halo_copy(n, d, row_src), "send")
            for h in TRIO:
                activate_row(n, h)
            sums = (None, zero8, zero8)
            for h, ahead in zip(EDGE, ((HE - 3, HE - 2, HE - 1), (3, 4))):
                conv(n, (h,), TAPS)
                for k in ahead:
                    activate_row(n, k)
                sums = finish(b, s, (h,), sums)
            fill_columns(EDGE)
            conv(n, INNER, TAPS[:EARLY])
            for_dirs(lambda d: halo_copy(n + 1, d, row_src), "start", ROW_DIRS)
            for h in INNER:
                conv(n, (h,), TAPS[EARLY:])
                sums = finish(b, s, (h,), sums)
            pivot, s1, s2 = sums

            @pl.when(n < 3)
            def _():
                send_stats(n + 1, pivot, s1, s2)

            fill_columns(INNER)
            for_dirs(lambda d: halo_copy(n + 1, d, row_src), "start", COL_DIRS)
            return carry

        lax.fori_loop(0, 4, stage, 0)

        lax.fori_loop(1, HE - 1, plain_row, 0)
        for_dirs(lambda d: halo_copy(4, d, row_src), "recv", ROW_DIRS)
        halo_rows(4)
        for h in (0, HE - 1):
            plain_row(h, 0)
        for_dirs(lambda d: halo_copy(4, d, row_src), "recv", COL_DIRS)
        lax.fori_loop(0, HE, plain_edges, 0)
        for_dirs(lambda d: halo_copy(4, d, row_src), "send")
        for n in range(4):
            for j in range(1, n_dev):
                stat_copy(n, j).wait_send()

    main()


def up_kernel(a_ref, wu, ub, out, o32, part, ob, o_sem):
    def out_copy(q, a, hp):
        return pltpu.make_async_copy(ob.at[hp, q, a], out.at[:, 2 * (q * 3 + hp) + a], o_sem.at[hp, q, a])

    def main(*accs):
        for acc in accs:
            pltpu.matmul_pop(acc)

        def row_taps(a):
            return [(1, 1)] if a is None else [(0, a), (2, a + 1)]

        groups = []
        for a in (None, 0, 1):
            for b in (None, 0, 1):
                groups.append((a, b, [(k, l, dh, kw) for k, dh in row_taps(a) for l, kw in row_taps(b)]))
        taps = [(g, tap) for g, grp in enumerate(groups) for tap in grp[2]]

        def push(i):
            k, l, _, _ = taps[i % len(taps)][1]
            for q in PAIR:
                pltpu.matmul_push_rhs(wu[k, l], staging_register=0, mxu_index=q, transpose=True)

        def blocks(q, slot):
            va = pltpu.matmul_pop(accs[q * 6 + slot * 2])
            vb = pltpu.matmul_pop(accs[q * 6 + slot * 2 + 1])
            return va, vb

        push(0)
        for hp in TRIO:
            for i, (g, (k, l, dh, kw)) in enumerate(taps):
                slot = g % 3
                for q in PAIR:
                    pltpu.matmul_acc_lhs(accs[q * 6 + slot * 2], a_ref[kw, q * 3 + hp + dh, pl.ds(32, NA), :], load_staged_rhs=0)
                if hp < 2 or i + 1 < len(taps):
                    push(i + 1)
                for q in PAIR:
                    pltpu.matmul_acc_lhs(accs[q * 6 + slot * 2 + 1], a_ref[kw, q * 3 + hp + dh, pl.ds(ABASE + 32, NB), :])
                if i + 1 < len(taps) and taps[i + 1][0] == g:
                    continue
                a, b, _ = groups[g]
                for q in PAIR:
                    va, vb = blocks(q, slot)
                    for v, sl in ((va, pl.ds(0, NA)), (vb, pl.ds(NA, NB))):
                        if a is None and b is None:
                            part[q, 0, sl, :] = v + ub[...]
                        elif a is None:
                            part[q, 1 + b, sl, :] = v + part[q, 0, sl, :]
                        elif b is None:
                            part[q, 3, sl, :] = v
                    if a is None or b is None:
                        continue
                    va = va + part[q, 1 + b, pl.ds(0, NA), :] + part[q, 3, pl.ds(0, NA), :]
                    vb = vb + part[q, 1 + b, pl.ds(NA, NB), :] + part[q, 3, pl.ds(NA, NB), :]
                    for half in PAIR:
                        ln = slice(half * LN, half * LN + LN)
                        for t in range(T):
                            o32[q, half, pl.ds(t * 2 * W + b, TR, stride=2), :] = va[t * TR:t * TR + TR, ln]
                            kb = (t % T2) * TR + (t // T2) * 8
                            o32[q, half, pl.ds(t * 48 + 32 + b, 8, stride=2), :] = vb[kb:kb + 8, ln]
                    if b == 1:
                        for t in range(T):
                            for half in PAIR:
                                ob[hp, q, a, t, :, lanes(half)] = o32[q, half, pl.ds(t * 2 * W, 2 * W), :].astype(BF16)
                        out_copy(q, a, hp).start()
        for hp in TRIO:
            for q in PAIR:
                for a in PAIR:
                    out_copy(q, a, hp).wait()

    pl.run_scoped(main, *acc_specs())


def solution(mesh):
    n_sh, n_sw = mesh.shape["sh"], mesh.shape["sw"]
    n_dev = n_sh * n_sw
    vmem = pl.BlockSpec(memory_space=pltpu.VMEM)
    hbm = pl.BlockSpec(memory_space=pltpu.HBM)
    dma = pltpu.SemaphoreType.DMA
    vec, mat = pltpu.VMEM((2, 2, C), F32), pltpu.VMEM((2, 2, LZ, C), BF16)

    def local_step(features, latent, gn_gain, gn_bias, zy_weight, zy_bias, zb_weight, zb_bias, conv_weight, conv_bias, up_weight, up_bias):
        feat = features[0].transpose(1, 2, 3, 0)
        lat = latent[0].transpose(1, 2, 0, 3)
        cw = conv_weight.transpose(0, 1, 4, 5, 6, 2, 3).reshape(2, 2, 27, C, C)
        uw = up_weight.transpose(2, 3, 0, 1)
        aup = pl.pallas_call(
            functools.partial(stage_kernel, n_sh, n_sw),
            out_shape=jax.ShapeDtypeStruct((3, HE, AR, C), BF16),
            in_specs=[hbm] * 10,
            out_specs=vmem,
            scratch_shapes=[
                pltpu.VMEM((4, 27, C, C), BF16),
                pltpu.VMEM((3, HE, AR, C), BF16),
                pltpu.VMEM((2, HE * FR, 128), F32),
                pltpu.VMEM((H, FR, C), F32),
                pltpu.VMEM((H, FR, C), F32),
                pltpu.VMEM((HE + 1, FR, C), F32),
                pltpu.VMEM((HE + 1, FR, C), F32),
                pltpu.VMEM((HE + 1, FR, 128), BF16),
                pltpu.VMEM((H * FR + 96, 128), F32),
                pltpu.VMEM((T, H, LZ, W), BF16),
                pltpu.VMEM((T, H, W, C), BF16),
                pltpu.VMEM((5, 2, T, W, C), BF16),
                pltpu.VMEM((5, 2, HE, 16, C), BF16),
                pltpu.VMEM((2, T, W, C), BF16),
                pltpu.VMEM((2, H, 16, C), BF16),
                pltpu.VMEM((2, H * 16, 128), BF16),
                pltpu.VMEM((HE, 2, T * SW_, LN), F32),
                pltpu.VMEM((LN, 2 * C), BF16),
                pltpu.VMEM((4, 1, LN), F32),
                pltpu.VMEM((4, n_dev, 1, LN), F32),
                pltpu.VMEM((3, 8, C), F32),
                vec, vec, mat, vec, mat, vec, vec,
                dma((9,)), dma((4,)), dma((5, 8)), dma((5, 8)), dma((8,)), dma((8,)), dma((4, n_dev)), dma((4, n_dev)),
            ],
            compiler_params=pltpu.CompilerParams(collective_id=0, has_side_effects=True, vmem_limit_bytes=42 << 20),
            name="stages",
        )(*[pltpu.with_memory_space_constraint(v, pltpu.HBM) for v in (feat, lat, gn_gain, gn_bias, zy_weight, zy_bias, zb_weight, zb_bias, cw, conv_bias)])
        out = pl.pallas_call(
            up_kernel,
            out_shape=jax.ShapeDtypeStruct((T, 2 * H, 2 * W, C), BF16),
            in_specs=[vmem] * 3,
            out_specs=hbm,
            scratch_shapes=[
                pltpu.VMEM((2, 2, T * 2 * W, LN), F32),
                pltpu.VMEM((2, 4, FR, C), F32),
                pltpu.VMEM((3, 2, 2, T, 2 * W, C), BF16),
                dma((3, 2, 2)),
            ],
            compiler_params=pltpu.CompilerParams(vmem_limit_bytes=24 << 20),
            name="upsample",
        )(aup, uw, up_bias.reshape(1, C))
        return out.transpose(3, 0, 1, 2)[None]

    data_spec = P("dp", None, None, "sh", "sw")
    return jax.shard_map(local_step, mesh=mesh, in_specs=(data_spec, data_spec) + (P(),) * 10, out_specs=data_spec, check_vma=False)
```
